256 devices in a mesh: table: 4 (over z_lo), row: 64 (over z_hi, y, x, core).
Axes of the slice: x: 4, y: 4, z: 8 (z_hi: 2, z_lo: 4; z = z_hi * 4 + z_lo), core: 2. Of those that a mesh axis runs over, the one named last changes fastest.
Arguments:
- tables: bfloat16 [4, 524288, 128], P('table', 'row'), may hold values from -3 to 3
- indices: int32 [4, 100, 512], P('table'), may hold values from 0 to 524287
- weights: bfloat16 [4, 100, 512], P('table'), may hold values from 0.19921875 to 1
- lengths: int32 [4, 512], P('table'), may hold values from 1 to 100, as said below
Outputs:
- pooled: bfloat16 [4, 512, 128], P(None, ('table', 'row'))
The draws below stay inside these ranges and needn't reach their ends.
Inputs may be any that keep to these rules, and one draw needn't show every extreme that they name: `lengths`: the longest bag of each table has a power of two of at most 64 positions, or 100 positions, and some table has a bag of 100.
All inputs are finite; a program needn't handle non-finite values.
Results may differ from the reference program's by a relative error of at most 0.001.
Values may be sent and summed in bfloat16 or wider, within the bound.
No kernel may reach another device: no remote copies, remote signals or barrier semaphores. Data moves between devices by JAX's collectives and lax.ppermute only.
A program may use at most 64 MiB of HBM per device.

```python
import math
import jax
import jax.numpy as jnp
import numpy as np
from jax import lax

D = 128
BAG = 100
NT = 4
ROWS = 524288
BATCH = 512


def draw_lengths(key, part):
    subkeys = jax.random.split(key, 4)
    exponent = jax.random.randint(subkeys[0], (NT, 1), 0, 8)
    table_caps = jnp.minimum(jnp.left_shift(jnp.ones_like(exponent), exponent), BAG)
    longest = jax.random.randint(subkeys[1], (), 0, NT)
    table_caps = jnp.where(jnp.arange(NT)[:, None] == longest, BAG, table_caps)
    uniform_draw = jax.random.randint(subkeys[2], (NT, BATCH), 0, 1 << 20)
    lengths = uniform_draw % table_caps + 1
    chosen = jax.random.randint(subkeys[3], (NT, 1), 0, BATCH)
    lengths = jnp.where(jnp.arange(BATCH)[None, :] == chosen, table_caps, lengths)
    return lengths.astype(jnp.int32)


def touch_ends(entries, key, least, largest):
    shape = entries.shape
    place = [jax.random.randint(jax.random.fold_in(key, axis), (), 0, shape[axis]) for axis in range(len(shape))]
    entries = entries.at[tuple(place)].set(least)
    longest = shape.index(max(shape))
    place[longest] = (place[longest] + 1) % shape[longest]
    return entries.at[tuple(place)].set(largest)


def block_scale(rng, extent, cuts, least, top_value):
    factor_of, own = 1.0, jax.random.fold_in(rng, 6)
    for dim, parts in cuts:
        heights = jnp.exp(jax.random.uniform(jax.random.fold_in(own, dim), (parts,), jnp.float32, least / len(cuts), top_value / len(cuts)))
        factor_of = factor_of * jnp.repeat(heights, extent[dim] // parts).reshape([-1 if axis == dim else 1 for axis in range(len(extent))])
    return factor_of


def wide_ids(own_key, dims, count, slope):
    loads = [min(1 << octave, count + 1 - (1 << octave)) * (1 << 20) // math.isqrt((1 << octave) ** slope) + 1 for octave in range((count + 1).bit_length()) if 1 << octave <= count]
    scale = 1 + sum(loads) // (1 << 30)
    grid = np.cumsum(np.array([max(1, weight // scale) for weight in loads]))
    lot = jax.random.randint(jax.random.fold_in(own_key, 1), dims, 0, int(grid[len(loads) - 1]))
    start = jnp.left_shift(1, jnp.searchsorted(jnp.asarray(grid, jnp.int32), lot, side="right").astype(jnp.int32))
    standing = start - 1 + jax.random.randint(jax.random.fold_in(own_key, 4), dims, 0, 1 << 30) % jnp.minimum(start, count + 1 - start)
    return jax.random.permutation(jax.random.fold_in(own_key, 2), count)[standing].astype(jnp.int32)


def noise(rng, shape, scale, most, cuts=(), kind=jnp.bfloat16):
    result = scale * jax.random.normal(rng, shape, jnp.float32)
    if cuts:
        result = result * block_scale(rng, shape, cuts, -0.22, 0.18)
    return jnp.clip(result, -most, most).astype(kind)


def setup_inputs(seed: int = 0) -> dict:
    key_list = jax.random.split(jax.random.key(seed), 5)
    return {
        "tables": noise(key_list[0], (NT, ROWS, D), 0.5, 3.0, ((0, 4), (1, 64))),
        "indices": touch_ends(wide_ids(key_list[1], (NT, BAG, BATCH), ROWS, 2), jax.random.fold_in(key_list[1], 3), 0, ROWS - 1).astype(jnp.int32),
        "weights": jnp.clip(0.19921875 + 0.80078125 * jax.random.uniform(key_list[2], (NT, BAG, BATCH), jnp.float32) ** block_scale(key_list[2], (NT, BAG, BATCH), ((0, 4),), -0.2, 0.2), 0.19921875, 1.0).astype(jnp.bfloat16),
        "lengths": draw_lengths(jax.random.fold_in(key_list[4], 71), 0),
    }


bag_block = 10


def pool_table(operands):
    table_rows, index_rows, weight, length = operands
    position = jnp.arange(BAG, dtype=jnp.int32)[:, None]
    factors = jnp.where(position < length[None, :], weight, jnp.zeros_like(weight))

    def add_block(running, first_row):
        index_block = lax.dynamic_slice_in_dim(index_rows, first_row, bag_block, 0)
        factor_block = lax.dynamic_slice_in_dim(factors, first_row, bag_block, 0)
        gathered = jnp.take(table_rows, index_block, axis=0)
        running = running + jnp.einsum("lb,lbd->bd", factor_block.astype(jnp.float32), gathered.astype(jnp.float32))
        return running, None

    starts = jnp.arange(0, BAG, bag_block, dtype=jnp.int32)
    running, unused = lax.scan(add_block, jnp.zeros((BATCH, D), jnp.float32), starts)
    return running.astype(jnp.bfloat16)


def reference(tables, indices, weights, lengths):
    return lax.map(pool_table, (tables, indices, weights, lengths))
```

```python
import functools

import jax
import jax.numpy as jnp
from jax import lax
from jax.experimental import pallas as pl
from jax.experimental.pallas import tpu as pltpu
from jax.sharding import PartitionSpec as P

lanes = 128
packed_rows = 16
bags_per_step = 8
bags_per_dot = 256


def pool_kernel(
    start_ref,
    index_ref,
    weight_ref,
    length_ref,
    table_hbm,
    out_ref,
    table_ref,
    high_ref,
    low_ref,
    factor_ref,
    spread_ref,
    table_sem,
):
    table_copy = pltpu.make_async_copy(table_hbm, table_ref, table_sem)
    table_copy.start()
    bag, batch = index_ref.shape
    rows = table_ref.shape[0]
    tiles = rows // lanes
    stride = spread_ref.shape[0] // tiles

    local = index_ref[...] - start_ref[0]
    position = lax.broadcasted_iota(jnp.int32, (bag, batch), 0)
    inside = (local >= 0) & (local < rows) & (position < length_ref[...])
    local = jnp.where(inside, local, -1).astype(jnp.float32)
    weight = weight_ref[...].astype(jnp.float32)
    pad = lanes - bag
    local = jnp.concatenate([local, jnp.full((pad, batch), -1.0, jnp.float32)], 0)
    weight = jnp.concatenate([weight, jnp.zeros((pad, batch), jnp.float32)], 0)
    local = local.T.astype(jnp.int32)
    high_ref[...] = (local >> 7).astype(jnp.float32)
    low_ref[...] = (local & (lanes - 1)).astype(jnp.float32)
    factor_ref[...] = weight.T

    row_id = lax.broadcasted_iota(jnp.int32, (packed_rows, lanes), 0)
    row_ids = [
        (row_id + packed_rows * j).astype(jnp.float32).astype(jnp.bfloat16)
        for j in range(lanes // packed_rows)
    ]
    zero = jnp.zeros((packed_rows, lanes), jnp.bfloat16)
    one = jnp.ones((packed_rows, lanes), jnp.bfloat16)

    def row_of(ref, bag_number):
        row = ref[pl.ds(bag_number, 1), :]
        return jnp.broadcast_to(row, (packed_rows, lanes)).astype(jnp.bfloat16)

    def spread_bag(bag_number):
        high = row_of(high_ref, bag_number)
        low = row_of(low_ref, bag_number)
        factor = row_of(factor_ref, bag_number)
        by_high = [jnp.where(high == ids, factor, zero) for ids in row_ids[: tiles // packed_rows]]
        by_low = [jnp.where(low == ids, one, zero) for ids in row_ids]
        return lax.dot_general(
            jnp.concatenate(by_high, 0),
            jnp.concatenate(by_low, 0),
            (((1,), (1,)), ((), ())),
            preferred_element_type=jnp.float32,
        )

    def spread_step(step, carry):
        for k in range(bags_per_step):
            bag_number = step * bags_per_step + k
            spread_ref[pl.ds(bag_number, tiles, stride=stride), :] = spread_bag(bag_number)
        return carry

    lax.fori_loop(0, batch // bags_per_step, spread_step, 0)
    table_copy.wait()
    for first in range(0, batch, bags_per_dot):
        factors = jnp.concatenate(
            [spread_ref[pl.ds(j * stride + first, bags_per_dot), :] for j in range(tiles)], 1
        )
        upper = factors.astype(jnp.bfloat16)
        rest = (factors - upper.astype(jnp.float32)).astype(jnp.bfloat16)
        table = table_ref[...]
        total = jnp.dot(upper, table, preferred_element_type=jnp.float32)
        total = total + jnp.dot(rest, table, preferred_element_type=jnp.float32)
        out_ref[pl.ds(first, bags_per_dot), :] = total


def pool_local(table_rows, index_rows, weight, length, row_start):
    rows, width = table_rows.shape
    batch = index_rows.shape[1]
    vmem = pl.BlockSpec(memory_space=pltpu.VMEM)
    return pl.pallas_call(
        pool_kernel,
        out_shape=jax.ShapeDtypeStruct((batch, width), jnp.float32),
        in_specs=[
            pl.BlockSpec(memory_space=pltpu.SMEM),
            vmem,
            vmem,
            vmem,
            pl.BlockSpec(memory_space=pl.ANY),
        ],
        out_specs=vmem,
        scratch_shapes=[
            pltpu.VMEM((rows, width), table_rows.dtype),
            pltpu.VMEM((batch, lanes), jnp.float32),
            pltpu.VMEM((batch, lanes), jnp.float32),
            pltpu.VMEM((batch, lanes), jnp.float32),
            pltpu.VMEM(((batch + 1) * (rows // lanes), lanes), jnp.float32),
            pltpu.SemaphoreType.DMA,
        ],
    )(row_start.reshape(1), index_rows, weight, length, table_rows)


def on_device(tables, indices, weights, lengths):
    _, row_dev, feature_width = tables.shape
    batch_size = indices.shape[2]
    table_count = lax.axis_size("table")
    row_count = lax.axis_size("row")
    row_start = (lax.axis_index("row") * row_dev).astype(jnp.int32)
    partial = pool_local(tables[0], indices[0], weights[0], lengths, row_start)
    share = batch_size // (table_count * row_count)
    tiles = partial.reshape(table_count * row_count, share, feature_width)
    arrived = lax.all_to_all(tiles, ("table", "row"), split_axis=0, concat_axis=0, tiled=True)
    shares = arrived.reshape(table_count, row_count, share, feature_width)
    return shares.sum(axis=1).astype(jnp.bfloat16)


def solution(mesh):
    placed = (
        P("table", "row", None),
        P("table", None, None),
        P("table", None, None),
        P("table", None),
    )
    return jax.shard_map(
        on_device,
        mesh=mesh,
        in_specs=placed,
        out_specs=P(None, ("table", "row"), None),
        check_vma=False,
    )
```

```python
import jax
import jax.numpy as jnp
from jax import lax
from jax.experimental import pallas as pl
from jax.experimental.pallas import tpu as pltpu
from jax.sharding import PartitionSpec as P

lanes = 128
packed_rows = 16
slots = 16
weight_unit = 1024
groups_per_step = 4
bags_per_dot = 256


def pool_kernel(
    start_ref,
    index_ref,
    weight_ref,
    length_ref,
    table_hbm,
    out_ref,
    table_ref,
    rank_ref,
    code_ref,
    high_ref,
    low_ref,
    factor_ref,
    spread_ref,
    table_sem,
):
    table_copy = pltpu.make_async_copy(table_hbm, table_ref, table_sem)
    table_copy.start()
    bag, _, batch = index_ref.shape
    rows = table_ref.shape[0]
    tiles = rows // lanes
    octets = tiles // 8
    stride = spread_ref.shape[0] // tiles
    blocks = batch // lanes
    padded = rank_ref.shape[0]
    groups = high_ref.shape[0]
    group_bags = lanes // slots

    local = index_ref[:, 0, :] - start_ref[0]
    position = lax.broadcasted_iota(jnp.int32, (bag, batch), 0)
    inside = (local >= 0) & (local < rows) & (position < length_ref[...])
    code = local.astype(jnp.float32) * (2.0 * weight_unit)
    code = code + weight_ref[...].astype(jnp.float32) * weight_unit
    code_ref[:bag, :] = jnp.where(inside, code, 0.0)
    code_ref[bag:, :] = jnp.zeros((padded - bag, batch), jnp.float32)

    used = jnp.where(inside, 1.0, 0.0)
    used = jnp.concatenate([used, jnp.zeros((lanes - bag, batch), jnp.float32)], 0)
    before = lax.broadcasted_iota(jnp.int32, (padded, lanes), 0) > lax.broadcasted_iota(
        jnp.int32, (padded, lanes), 1
    )
    rank = jnp.dot(
        jnp.where(before, 1.0, 0.0).astype(jnp.bfloat16),
        used.astype(jnp.bfloat16),
        preferred_element_type=jnp.float32,
    )
    rank_ref[...] = rank
    rounds = (jnp.max(rank[padded - 1 :, :]).astype(jnp.int32) + (slots - 1)) // slots

    row_id = lax.broadcasted_iota(jnp.int32, (packed_rows, lanes), 0)
    row_ids = [
        (row_id + packed_rows * i).astype(jnp.float32).astype(jnp.bfloat16)
        for i in range(lanes // packed_rows)
    ]
    zero = jnp.zeros((packed_rows, lanes), jnp.bfloat16)
    one = jnp.ones((packed_rows, lanes), jnp.bfloat16)
    owner = lax.broadcasted_iota(jnp.int32, (packed_rows, lanes), 1) // slots
    owner = owner.astype(jnp.float32).astype(jnp.bfloat16)
    owned = [owner == jnp.full_like(owner, g) for g in range(group_bags)]

    def fill_slots(first):
        planes = []
        for block in range(blocks):
            where = pl.ds(block * lanes, lanes)
            rank = rank_ref[:, where]
            code = code_ref[:, where]
            for s in range(slots):
                at = rank == (first + s).astype(jnp.float32)
                planes.append(jnp.sum(jnp.where(at, code, 0.0), axis=0, keepdims=True))
        plane = jnp.concatenate(planes, 0)
        plane = jnp.concatenate([plane, pltpu.roll(plane, lanes - groups, 1)], 0)
        code = plane.T[:groups].astype(jnp.int32)
        row = code // (2 * weight_unit)
        high_ref[...] = (row // lanes).astype(jnp.float32)
        low_ref[...] = (row % lanes).astype(jnp.float32)
        factor = (code % (2 * weight_unit)).astype(jnp.float32)
        factor_ref[...] = factor * (1.0 / weight_unit)

    def row_of(ref, j):
        row = ref[pl.ds(j, 1), :]
        return jnp.broadcast_to(row, (packed_rows, lanes)).astype(jnp.bfloat16)

    def spread_group(j):
        high = row_of(high_ref, j)
        low = row_of(low_ref, j)
        factor = row_of(factor_ref, j)
        at = [high == ids for ids in row_ids[: tiles // packed_rows]]
        by_high = []
        for g in range(group_bags):
            mine = jnp.where(owned[g], factor, zero)
            by_high += [jnp.where(hit, mine, zero) for hit in at]
        by_low = [jnp.where(low == ids, one, zero) for ids in row_ids]
        return lax.dot_general(
            jnp.concatenate(by_high, 0),
            jnp.concatenate(by_low, 0),
            (((1,), (1,)), ((), ())),
            preferred_element_type=jnp.float32,
        )

    def spread_step(step, inexact, add):
        inexact = list(inexact)
        for k in range(groups_per_step):
            j = step * groups_per_step + k
            total = spread_group(j)
            for g in range(group_bags):
                first = (g % blocks) * lanes + (g // blocks) * groups
                where = pl.ds(first + j, tiles, stride=stride)
                part = total[g * tiles : (g + 1) * tiles]
                if add:
                    part = part + spread_ref[where, :]
                spread_ref[where, :] = part
                rest = jnp.abs(part - part.astype(jnp.bfloat16).astype(jnp.float32))
                for o in range(octets):
                    inexact[o] = jnp.maximum(inexact[o], rest[o * 8 : (o + 1) * 8])
        return tuple(inexact)

    def spread_round(inexact, add):
        return lax.fori_loop(
            0,
            groups // groups_per_step,
            lambda step, found: spread_step(step, found, add),
            inexact,
        )

    def later_round(number, inexact):
        fill_slots(number * slots)
        return spread_round(inexact, True)

    fill_slots(jnp.int32(0))
    inexact = tuple(jnp.zeros((8, lanes), jnp.float32) for _ in range(octets))
    inexact = spread_round(inexact, False)
    inexact = lax.fori_loop(1, rounds, later_round, inexact)

    table_copy.wait()
    for first in range(0, batch, bags_per_dot):
        factors = [
            spread_ref[pl.ds(i * stride + first, bags_per_dot), :].astype(jnp.bfloat16)
            for i in range(tiles)
        ]
        out_ref[pl.ds(first, bags_per_dot), :] = jnp.dot(
            jnp.concatenate(factors, 1), table_ref[...], preferred_element_type=jnp.float32
        )

    for o in range(octets):

        @pl.when(jnp.max(inexact[o]) > 0)
        def _(o=o):
            factors = jnp.concatenate(
                [spread_ref[pl.ds((8 * o + i) * stride, batch), :] for i in range(8)], 1
            )
            rest = factors - factors.astype(jnp.bfloat16).astype(jnp.float32)
            out_ref[...] += jnp.dot(
                rest.astype(jnp.bfloat16),
                table_ref[pl.ds(8 * o * lanes, 8 * lanes), :],
                preferred_element_type=jnp.float32,
            )


def pool_local(table_rows, index_rows, weight, length, row_start):
    rows, width = table_rows.shape
    bag, batch = weight.shape
    padded = bag + 8 - bag % 8
    groups = batch * slots // lanes
    vmem = pl.BlockSpec(memory_space=pltpu.VMEM)
    by_position = pltpu.VMEM((padded, batch), jnp.float32)
    by_group = pltpu.VMEM((groups, lanes), jnp.float32)
    return pl.pallas_call(
        pool_kernel,
        out_shape=jax.ShapeDtypeStruct((batch, width), jnp.float32),
        in_specs=[
            pl.BlockSpec(memory_space=pltpu.SMEM),
            vmem,
            vmem,
            vmem,
            pl.BlockSpec(memory_space=pl.ANY),
        ],
        out_specs=vmem,
        scratch_shapes=[
            pltpu.VMEM((rows, width), table_rows.dtype),
            by_position,
            by_position,
            by_group,
            by_group,
            by_group,
            pltpu.VMEM(((batch + 1) * (rows // lanes), lanes), jnp.float32),
            pltpu.SemaphoreType.DMA,
        ],
    )(row_start.reshape(1), index_rows, weight, length, table_rows)


def on_device(tables, indices, weights, lengths):
    _, row_dev, feature_width = tables.shape
    batch_size = indices.shape[2]
    table_count = lax.axis_size("table")
    row_count = lax.axis_size("row")
    row_start = (lax.axis_index("row") * row_dev).astype(jnp.int32)
    index_rows = indices.transpose(1, 0, 2)
    partial = pool_local(tables[0], index_rows, weights[0], lengths, row_start)
    share = batch_size // (table_count * row_count)
    tiles = partial.reshape(table_count * row_count, share, feature_width)
    arrived = lax.all_to_all(tiles, ("table", "row"), split_axis=0, concat_axis=0, tiled=True)
    shares = arrived.reshape(table_count, row_count, share, feature_width)
    return shares.sum(axis=1).astype(jnp.bfloat16)


def solution(mesh):
    placed = (
        P("table", "row", None),
        P("table", None, None),
        P("table", None, None),
        P("table", None),
    )
    return jax.shard_map(
        on_device,
        mesh=mesh,
        in_specs=placed,
        out_specs=P(None, ("table", "row"), None),
        check_vma=False,
    )
```

```python
import jax
import jax.numpy as jnp
from jax import lax
from jax.experimental import pallas as pl
from jax.experimental.pallas import tpu as pltpu
from jax.sharding import PartitionSpec as P

lanes = 128
packed_rows = 16
slots = 16
weight_unit = 1024
groups_per_step = 32
vmem_bytes = 24 * 2**20
bags_per_dot = 256


def pool_kernel(
    start_ref,
    index_ref,
    weight_ref,
    length_ref,
    table_hbm,
    out_ref,
    table_ref,
    rank_ref,
    code_ref,
    high_ref,
    low_ref,
    factor_ref,
    spread_ref,
    table_sem,
):
    table_copy = pltpu.make_async_copy(table_hbm, table_ref, table_sem)
    table_copy.start()
    bag, _, batch = index_ref.shape
    rows = table_ref.shape[0]
    tiles = rows // lanes
    octets = tiles // 8
    stride = spread_ref.shape[0] // tiles
    blocks = batch // lanes
    padded = rank_ref.shape[0]
    groups = high_ref.shape[0]
    group_bags = lanes // slots

    local = index_ref[:, 0, :] - start_ref[0]
    position = lax.broadcasted_iota(jnp.int32, (bag, batch), 0)
    inside = (local >= 0) & (local < rows) & (position < length_ref[...])
    code = local.astype(jnp.float32) * (2.0 * weight_unit)
    code = code + weight_ref[...].astype(jnp.float32) * weight_unit
    code_ref[:bag, :] = jnp.where(inside, code, 0.0)
    code_ref[bag:, :] = jnp.zeros((padded - bag, batch), jnp.float32)

    used = jnp.where(inside, 1.0, 0.0)
    used = jnp.concatenate([used, jnp.zeros((lanes - bag, batch), jnp.float32)], 0)
    before = lax.broadcasted_iota(jnp.int32, (padded, lanes), 0) > lax.broadcasted_iota(
        jnp.int32, (padded, lanes), 1
    )
    rank = jnp.dot(
        jnp.where(before, 1.0, 0.0).astype(jnp.bfloat16),
        used.astype(jnp.bfloat16),
        preferred_element_type=jnp.float32,
    )
    rank_ref[...] = rank
    rounds = (jnp.max(rank[padded - 1 :, :]).astype(jnp.int32) + (slots - 1)) // slots

    row_id = lax.broadcasted_iota(jnp.int32, (packed_rows, lanes), 0)
    row_ids = [
        (row_id + packed_rows * i).astype(jnp.float32).astype(jnp.bfloat16)
        for i in range(lanes // packed_rows)
    ]
    zero = jnp.zeros((packed_rows, lanes), jnp.bfloat16)
    one = jnp.ones((packed_rows, lanes), jnp.bfloat16)
    owner = lax.broadcasted_iota(jnp.int32, (packed_rows, lanes), 1) // slots
    owner = owner.astype(jnp.float32).astype(jnp.bfloat16)
    owned = [owner == jnp.full_like(owner, g) for g in range(group_bags)]

    def fill_slots(first):
        planes = []
        for block in range(blocks):
            where = pl.ds(block * lanes, lanes)
            rank = rank_ref[:, where]
            code = code_ref[:, where]
            for s in range(slots):
                at = rank == (first + s).astype(jnp.float32)
                planes.append(jnp.sum(jnp.where(at, code, 0.0), axis=0, keepdims=True))
        plane = jnp.concatenate(planes, 0)
        plane = jnp.concatenate([plane, pltpu.roll(plane, lanes - groups, 1)], 0)
        code = plane.T[:groups].astype(jnp.int32)
        row = code // (2 * weight_unit)
        high_ref[...] = (row // lanes).astype(jnp.float32)
        low_ref[...] = (row % lanes).astype(jnp.float32)
        factor = (code % (2 * weight_unit)).astype(jnp.float32)
        factor_ref[...] = factor * (1.0 / weight_unit)

    def row_of(ref, j):
        row = ref[pl.ds(j, 1), :]
        return jnp.broadcast_to(row, (packed_rows, lanes)).astype(jnp.bfloat16)

    def spread_group(j):
        high = row_of(high_ref, j)
        low = row_of(low_ref, j)
        factor = row_of(factor_ref, j)
        at = [high == ids for ids in row_ids[: tiles // packed_rows]]
        by_high = []
        for g in range(group_bags):
            mine = jnp.where(owned[g], factor, zero)
            by_high += [jnp.where(hit, mine, zero) for hit in at]
        by_low = [jnp.where(low == ids, one, zero) for ids in row_ids]
        return lax.dot_general(
            jnp.concatenate(by_high, 0),
            jnp.concatenate(by_low, 0),
            (((1,), (1,)), ((), ())),
            preferred_element_type=jnp.float32,
        )

    def spread_step(step, inexact, add):
        inexact = list(inexact)
        for k in range(groups_per_step):
            j = step * groups_per_step + k
            total = spread_group(j)
            for g in range(group_bags):
                first = (g % blocks) * lanes + (g // blocks) * groups
                where = pl.ds(first + j, tiles, stride=stride)
                part = total[g * tiles : (g + 1) * tiles]
                if add:
                    part = part + spread_ref[where, :]
                spread_ref[where, :] = part
                rest = jnp.abs(part - part.astype(jnp.bfloat16).astype(jnp.float32))
                for o in range(octets):
                    inexact[o] = jnp.maximum(inexact[o], rest[o * 8 : (o + 1) * 8])
        return tuple(inexact)

    def spread_round(inexact, add):
        return lax.fori_loop(
            0,
            groups // groups_per_step,
            lambda step, found: spread_step(step, found, add),
            inexact,
        )

    def later_round(number, inexact):
        fill_slots(number * slots)
        return spread_round(inexact, True)

    fill_slots(jnp.int32(0))
    inexact = tuple(jnp.zeros((8, lanes), jnp.float32) for _ in range(octets))
    inexact = spread_round(inexact, False)
    inexact = lax.fori_loop(1, rounds, later_round, inexact)

    table_copy.wait()
    for first in range(0, batch, bags_per_dot):
        factors = [
            spread_ref[pl.ds(i * stride + first, bags_per_dot), :].astype(jnp.bfloat16)
            for i in range(tiles)
        ]
        out_ref[pl.ds(first, bags_per_dot), :] = jnp.dot(
            jnp.concatenate(factors, 1), table_ref[...], preferred_element_type=jnp.float32
        )

    for o in range(octets):

        @pl.when(jnp.max(inexact[o]) > 0)
        def _(o=o):
            factors = jnp.concatenate(
                [spread_ref[pl.ds((8 * o + i) * stride, batch), :] for i in range(8)], 1
            )
            rest = factors - factors.astype(jnp.bfloat16).astype(jnp.float32)
            out_ref[...] += jnp.dot(
                rest.astype(jnp.bfloat16),
                table_ref[pl.ds(8 * o * lanes, 8 * lanes), :],
                preferred_element_type=jnp.float32,
            )


def pool_local(table_rows, index_rows, weight, length, row_start):
    rows, width = table_rows.shape
    bag, batch = weight.shape
    padded = bag + 8 - bag % 8
    groups = batch * slots // lanes
    vmem = pl.BlockSpec(memory_space=pltpu.VMEM)
    by_position = pltpu.VMEM((padded, batch), jnp.float32)
    by_group = pltpu.VMEM((groups, lanes), jnp.float32)
    return pl.pallas_call(
        pool_kernel,
        out_shape=jax.ShapeDtypeStruct((batch, width), jnp.float32),
        in_specs=[
            pl.BlockSpec(memory_space=pltpu.SMEM),
            vmem,
            vmem,
            vmem,
            pl.BlockSpec(memory_space=pltpu.HBM),
        ],
        out_specs=vmem,
        scratch_shapes=[
            pltpu.VMEM((rows, width), table_rows.dtype),
            by_position,
            by_position,
            by_group,
            by_group,
            by_group,
            pltpu.VMEM(((batch + 1) * (rows // lanes), lanes), jnp.float32),
            pltpu.SemaphoreType.DMA,
        ],
        compiler_params=pltpu.CompilerParams(vmem_limit_bytes=vmem_bytes),
    )(row_start.reshape(1), index_rows, weight, length, table_rows)


def on_device(tables, indices, weights, lengths):
    _, row_dev, feature_width = tables.shape
    batch_size = indices.shape[2]
    table_count = lax.axis_size("table")
    row_count = lax.axis_size("row")
    row_start = (lax.axis_index("row") * row_dev).astype(jnp.int32)
    index_rows = indices.transpose(1, 0, 2)
    partial = pool_local(tables[0], index_rows, weights[0], lengths, row_start)
    share = batch_size // (table_count * row_count)
    tiles = partial.reshape(table_count * row_count, share, feature_width)
    arrived = lax.all_to_all(tiles, ("table", "row"), split_axis=0, concat_axis=0, tiled=True)
    shares = arrived.reshape(table_count, row_count, share, feature_width)
    return shares.sum(axis=1).astype(jnp.bfloat16)


def solution(mesh):
    placed = (
        P("table", "row", None),
        P("table", None, None),
        P("table", None, None),
        P("table", None),
    )
    return jax.shard_map(
        on_device,
        mesh=mesh,
        in_specs=placed,
        out_specs=P(None, ("table", "row"), None),
        check_vma=False,
    )
```

```python
import jax
import jax.numpy as jnp
from jax import lax
from jax.experimental import pallas as pl
from jax.experimental.pallas import tpu as pltpu
from jax.sharding import PartitionSpec as P

lanes = 128
packed_rows = 16
slots = 16
weight_unit = 1024
groups_per_step = 32
bags_per_dot = 256


def pool_kernel(
    start_ref,
    index_ref,
    weight_ref,
    length_ref,
    table_hbm,
    out_ref,
    table_ref,
    rank_ref,
    code_ref,
    high_ref,
    low_ref,
    factor_ref,
    spread_ref,
    table_sem,
):
    table_copy = pltpu.make_async_copy(table_hbm, table_ref, table_sem)
    table_copy.start()
    bag, _, batch = index_ref.shape
    rows = table_ref.shape[0]
    tiles = rows // lanes
    octets = tiles // 8
    stride = spread_ref.shape[0] // tiles
    blocks = batch // lanes
    padded = rank_ref.shape[0]
    groups = high_ref.shape[0]
    group_bags = lanes // slots

    local = index_ref[:, 0, :] - start_ref[0]
    position = lax.broadcasted_iota(jnp.int32, (bag, batch), 0)
    inside = (local >= 0) & (local < rows) & (position < length_ref[...])
    code = local.astype(jnp.float32) * (2.0 * weight_unit)
    code = code + weight_ref[...].astype(jnp.float32) * weight_unit
    code_ref[:bag, :] = jnp.where(inside, code, 0.0)
    code_ref[bag:, :] = jnp.zeros((padded - bag, batch), jnp.float32)

    used = jnp.where(inside, 1.0, 0.0)
    used = jnp.concatenate([used, jnp.zeros((lanes - bag, batch), jnp.float32)], 0)
    before = lax.broadcasted_iota(jnp.int32, (padded, lanes), 0) > lax.broadcasted_iota(
        jnp.int32, (padded, lanes), 1
    )
    rank = jnp.dot(
        jnp.where(before, 1.0, 0.0).astype(jnp.bfloat16),
        used.astype(jnp.bfloat16),
        preferred_element_type=jnp.float32,
    )
    rank_ref[...] = rank
    rounds = (jnp.max(rank[padded - 1 :, :]).astype(jnp.int32) + (slots - 1)) // slots

    row_id = lax.broadcasted_iota(jnp.int32, (packed_rows, lanes), 0)
    row_ids = [
        (row_id + packed_rows * i).astype(jnp.float32).astype(jnp.bfloat16)
        for i in range(lanes // packed_rows)
    ]
    zero = jnp.zeros((packed_rows, lanes), jnp.bfloat16)
    one = jnp.ones((packed_rows, lanes), jnp.bfloat16)
    owner = lax.broadcasted_iota(jnp.int32, (packed_rows, lanes), 1) // slots
    owner = owner.astype(jnp.float32).astype(jnp.bfloat16)
    owned = [owner == jnp.full_like(owner, g) for g in range(group_bags)]

    def fill_slots(first):
        planes = []
        for block in range(blocks):
            where = pl.ds(block * lanes, lanes)
            rank = rank_ref[:, where]
            code = code_ref[:, where]
            for s in range(slots):
                at = rank == (first + s).astype(jnp.float32)
                planes.append(jnp.sum(jnp.where(at, code, 0.0), axis=0, keepdims=True))
        plane = jnp.concatenate(planes, 0)
        plane = jnp.concatenate([plane, pltpu.roll(plane, lanes - groups, 1)], 0)
        code = plane.T[:groups].astype(jnp.int32)
        row = code // (2 * weight_unit)
        high_ref[...] = (row // lanes).astype(jnp.float32)
        low_ref[...] = (row % lanes).astype(jnp.float32)
        factor = (code % (2 * weight_unit)).astype(jnp.float32)
        factor_ref[...] = factor * (1.0 / weight_unit)

    def row_of(ref, j):
        row = ref[pl.ds(j, 1), :]
        return jnp.broadcast_to(row, (packed_rows, lanes)).astype(jnp.bfloat16)

    def spread_group(j):
        high = row_of(high_ref, j)
        low = row_of(low_ref, j)
        factor = row_of(factor_ref, j)
        at = [high == ids for ids in row_ids[: tiles // packed_rows]]
        by_high = []
        for g in range(group_bags):
            mine = jnp.where(owned[g], factor, zero)
            by_high += [jnp.where(hit, mine, zero) for hit in at]
        by_low = [jnp.where(low == ids, one, zero) for ids in row_ids]
        return lax.dot_general(
            jnp.concatenate(by_high, 0),
            jnp.concatenate(by_low, 0),
            (((1,), (1,)), ((), ())),
            preferred_element_type=jnp.float32,
        )

    def spread_step(step, inexact, add):
        inexact = list(inexact)
        for k in range(groups_per_step):
            j = step * groups_per_step + k
            total = spread_group(j)
            for g in range(group_bags):
                first = (g % blocks) * lanes + (g // blocks) * groups
                where = pl.ds(first + j, tiles, stride=stride)
                part = total[g * tiles : (g + 1) * tiles]
                if add:
                    part = part + spread_ref[where, :]
                spread_ref[where, :] = part
                rest = jnp.abs(part - part.astype(jnp.bfloat16).astype(jnp.float32))
                for o in range(octets):
                    inexact[o] = jnp.maximum(inexact[o], rest[o * 8 : (o + 1) * 8])
        return tuple(inexact)

    def spread_round(inexact, add):
        return lax.fori_loop(
            0,
            groups // groups_per_step,
            lambda step, found: spread_step(step, found, add),
            inexact,
        )

    def later_round(number, inexact):
        fill_slots(number * slots)
        return spread_round(inexact, True)

    fill_slots(jnp.int32(0))
    inexact = tuple(jnp.zeros((8, lanes), jnp.float32) for _ in range(octets))
    inexact = spread_round(inexact, False)
    inexact = lax.fori_loop(1, rounds, later_round, inexact)

    table_copy.wait()
    for first in range(0, batch, bags_per_dot):
        factors = [
            spread_ref[pl.ds(i * stride + first, bags_per_dot), :].astype(jnp.bfloat16)
            for i in range(tiles)
        ]
        out_ref[pl.ds(first, bags_per_dot), :] = jnp.dot(
            jnp.concatenate(factors, 1), table_ref[...], preferred_element_type=jnp.float32
        )

    for o in range(octets):

        @pl.when(jnp.max(inexact[o]) > 0)
        def _(o=o):
            factors = jnp.concatenate(
                [spread_ref[pl.ds((8 * o + i) * stride, batch), :] for i in range(8)], 1
            )
            rest = factors - factors.astype(jnp.bfloat16).astype(jnp.float32)
            out_ref[...] += jnp.dot(
                rest.astype(jnp.bfloat16),
                table_ref[pl.ds(8 * o * lanes, 8 * lanes), :],
                preferred_element_type=jnp.float32,
            )


def pool_local(table_rows, index_rows, weight, length, row_start):
    rows, width = table_rows.shape
    bag, batch = weight.shape
    padded = bag + 8 - bag % 8
    groups = batch * slots // lanes
    vmem = pl.BlockSpec(memory_space=pltpu.VMEM)
    by_position = pltpu.VMEM((padded, batch), jnp.float32)
    by_group = pltpu.VMEM((groups, lanes), jnp.float32)
    return pl.pallas_call(
        pool_kernel,
        out_shape=jax.ShapeDtypeStruct((batch, width), jnp.float32),
        in_specs=[
            pl.BlockSpec(memory_space=pltpu.SMEM),
            vmem,
            vmem,
            vmem,
            pl.BlockSpec(memory_space=pl.ANY),
        ],
        out_specs=vmem,
        scratch_shapes=[
            pltpu.VMEM((rows, width), table_rows.dtype),
            by_position,
            by_position,
            by_group,
            by_group,
            by_group,
            pltpu.VMEM(((batch + 1) * (rows // lanes), lanes), jnp.float32),
            pltpu.SemaphoreType.DMA,
        ],
    )(row_start.reshape(1), index_rows, weight, length, table_rows)


def on_device(tables, indices, weights, lengths):
    _, row_dev, feature_width = tables.shape
    batch_size = indices.shape[2]
    table_count = lax.axis_size("table")
    row_count = lax.axis_size("row")
    row_start = (lax.axis_index("row") * row_dev).astype(jnp.int32)
    index_rows = indices.transpose(1, 0, 2)
    partial = pool_local(tables[0], index_rows, weights[0], lengths, row_start)
    share = batch_size // (table_count * row_count)
    tiles = partial.reshape(table_count * row_count, share, feature_width)
    arrived = lax.all_to_all(tiles, ("table", "row"), split_axis=0, concat_axis=0, tiled=True)
    shares = arrived.reshape(table_count, row_count, share, feature_width)
    return shares.sum(axis=1).astype(jnp.bfloat16)


def solution(mesh):
    placed = (
        P("table", "row", None),
        P("table", None, None),
        P("table", None, None),
        P("table", None),
    )
    return jax.shard_map(
        on_device,
        mesh=mesh,
        in_specs=placed,
        out_specs=P(None, ("table", "row"), None),
        check_vma=False,
    )
```

```python
import jax
import jax.numpy as jnp
from jax import lax
from jax.experimental import pallas as pl
from jax.experimental.pallas import tpu as pltpu
from jax.sharding import Mesh
from jax.sharding import PartitionSpec as P

lanes = 128
packed_rows = 16
slots = 16
weight_unit = 1024


def read_positions(start_ref, index_ref, weight_ref, length_ref, rank_ref, code_ref, rows):
    bag, _, batch = index_ref.shape
    padded = rank_ref.shape[0]
    local = index_ref[:, 0, :] - start_ref[0]
    position = lax.broadcasted_iota(jnp.int32, (bag, batch), 0)
    inside = (local >= 0) & (local < rows) & (position < length_ref[...])
    code = local.astype(jnp.float32) * (2.0 * weight_unit)
    code = code + weight_ref[...].astype(jnp.float32) * weight_unit
    code_ref[:bag, :] = jnp.where(inside, code, 0.0)
    code_ref[bag:, :] = jnp.zeros((padded - bag, batch), jnp.float32)

    used = jnp.where(inside, 1.0, 0.0)
    used = jnp.concatenate([used, jnp.zeros((lanes - bag, batch), jnp.float32)], 0)
    before = lax.broadcasted_iota(jnp.int32, (padded, lanes), 0) > lax.broadcasted_iota(
        jnp.int32, (padded, lanes), 1
    )
    rank = jnp.dot(
        jnp.where(before, 1.0, 0.0).astype(jnp.bfloat16),
        used.astype(jnp.bfloat16),
        preferred_element_type=jnp.float32,
    )
    rank_ref[...] = rank
    return (jnp.max(rank[padded - 1 :, :]).astype(jnp.int32) + (slots - 1)) // slots


def fill_slots(rank_ref, code_ref, slot_refs, first):
    high_ref, low_ref, factor_ref = slot_refs
    groups = high_ref.shape[0]
    planes = []
    for block in range(rank_ref.shape[1] // lanes):
        where = pl.ds(block * lanes, lanes)
        rank = rank_ref[:, where]
        code = code_ref[:, where]
        for s in range(slots):
            at = rank == (first + s).astype(jnp.float32)
            planes.append(jnp.sum(jnp.where(at, code, 0.0), axis=0, keepdims=True))
    plane = jnp.concatenate(planes, 0)
    plane = jnp.concatenate([plane, pltpu.roll(plane, lanes - groups, 1)], 0)
    code = plane.T[:groups].astype(jnp.int32)
    row = code // (2 * weight_unit)
    high_ref[...] = (row // lanes).astype(jnp.float32)
    low_ref[...] = (row % lanes).astype(jnp.float32)
    factor = (code % (2 * weight_unit)).astype(jnp.float32)
    factor_ref[...] = factor * (1.0 / weight_unit)


def spread_half(slot_refs, spread_ref, core, tiles, inexact, add):
    high_ref, low_ref, factor_ref = slot_refs
    group_bags = lanes // slots
    half_groups = high_ref.shape[0] // 2
    stride = spread_ref.shape[0] // tiles
    row_id = lax.broadcasted_iota(jnp.int32, (packed_rows, lanes), 0)
    row_ids = [
        (row_id + packed_rows * i).astype(jnp.float32).astype(jnp.bfloat16)
        for i in range(lanes // packed_rows)
    ]
    zero = jnp.zeros((packed_rows, lanes), jnp.bfloat16)
    one = jnp.ones((packed_rows, lanes), jnp.bfloat16)
    owner = lax.broadcasted_iota(jnp.int32, (packed_rows, lanes), 1) // slots
    owner = owner.astype(jnp.float32).astype(jnp.bfloat16)
    owned = [owner == jnp.full_like(owner, g) for g in range(group_bags)]
    inexact = list(inexact)

    def row_of(ref, j):
        row = ref[pl.ds(j, 1), :]
        return jnp.broadcast_to(row, (packed_rows, lanes)).astype(jnp.bfloat16)

    for t in range(half_groups):
        j = t // 2 * 4 + t % 2 + 2 * core
        high = row_of(high_ref, j)
        low = row_of(low_ref, j)
        factor = row_of(factor_ref, j)
        at = [high == ids for ids in row_ids[: tiles // packed_rows]]
        by_high = []
        for g in range(group_bags):
            mine = jnp.where(owned[g], factor, zero)
            by_high += [jnp.where(hit, mine, zero) for hit in at]
        by_low = [jnp.where(low == ids, one, zero) for ids in row_ids]
        total = lax.dot_general(
            jnp.concatenate(by_high, 0),
            jnp.concatenate(by_low, 0),
            (((1,), (1,)), ((), ())),
            preferred_element_type=jnp.float32,
        )
        blocks = group_bags // 2
        for g in range(group_bags):
            first = (g % blocks * 2 + g // blocks) * half_groups
            where = pl.ds(first + t, tiles, stride=stride)
            part = total[g * tiles : (g + 1) * tiles]
            if add:
                part = part + spread_ref[where, :]
            spread_ref[where, :] = part
            rest = jnp.abs(part - part.astype(jnp.bfloat16).astype(jnp.float32))
            for o in range(len(inexact)):
                inexact[o] = jnp.maximum(inexact[o], rest[o * 8 : (o + 1) * 8])
    return tuple(inexact)


def multiply(spread_ref, table_ref, inexact, out_ref):
    tiles = table_ref.shape[0] // lanes
    stride = spread_ref.shape[0] // tiles
    bags = out_ref.shape[0]
    factors = [
        spread_ref[pl.ds(i * stride, bags), :].astype(jnp.bfloat16) for i in range(tiles)
    ]
    out_ref[...] = jnp.dot(
        jnp.concatenate(factors, 1), table_ref[...], preferred_element_type=jnp.float32
    )

    for o in range(len(inexact)):

        @pl.when(jnp.max(inexact[o]) > 0)
        def _(o=o):
            factors = jnp.concatenate(
                [spread_ref[pl.ds((8 * o + i) * stride, bags), :] for i in range(8)], 1
            )
            rest = factors - factors.astype(jnp.bfloat16).astype(jnp.float32)
            out_ref[...] += jnp.dot(
                rest.astype(jnp.bfloat16),
                table_ref[pl.ds(8 * o * lanes, 8 * lanes), :],
                preferred_element_type=jnp.float32,
            )


def exact_so_far(tiles):
    return tuple(jnp.zeros((8, lanes), jnp.float32) for _ in range(tiles // 8))


def send_kernel(
    start_ref,
    core_ref,
    index_ref,
    weight_ref,
    length_ref,
    table_hbm,
    out_ref,
    high_ref,
    low_ref,
    factor_ref,
    rounds_ref,
    table_ref,
    rank_ref,
    code_ref,
    high_later,
    low_later,
    factor_later,
    spread_ref,
    table_sem,
):
    table_copy = pltpu.make_async_copy(table_hbm, table_ref, table_sem)
    table_copy.start()
    rows = table_ref.shape[0]
    tiles = rows // lanes
    core = 1 - core_ref[0]
    rounds = read_positions(
        start_ref, index_ref, weight_ref, length_ref, rank_ref, code_ref, rows
    )
    rounds_ref[0] = rounds
    slot_refs = (high_ref, low_ref, factor_ref)
    later_refs = (high_later, low_later, factor_later)
    fill_slots(rank_ref, code_ref, slot_refs, jnp.int32(0))
    inexact = spread_half(slot_refs, spread_ref, core, tiles, exact_so_far(tiles), False)

    def later_round(number, inexact):
        fill_slots(rank_ref, code_ref, later_refs, number * slots)
        return spread_half(later_refs, spread_ref, core, tiles, inexact, True)

    inexact = lax.fori_loop(1, rounds, later_round, inexact)
    table_copy.wait()
    multiply(spread_ref, table_ref, inexact, out_ref)


def keep_kernel(
    start_ref,
    core_ref,
    rounds_ref,
    high_ref,
    low_ref,
    factor_ref,
    index_hbm,
    weight_hbm,
    length_hbm,
    table_hbm,
    out_ref,
    table_ref,
    index_ref,
    weight_ref,
    length_ref,
    rank_ref,
    code_ref,
    high_later,
    low_later,
    factor_later,
    spread_ref,
    table_sem,
    index_sem,
    weight_sem,
    length_sem,
):
    table_copy = pltpu.make_async_copy(table_hbm, table_ref, table_sem)
    table_copy.start()
    rows = table_ref.shape[0]
    tiles = rows // lanes
    core = core_ref[0]
    slot_refs = (high_ref, low_ref, factor_ref)
    later_refs = (high_later, low_later, factor_later)
    inexact = spread_half(slot_refs, spread_ref, core, tiles, exact_so_far(tiles), False)
    rounds = rounds_ref[0]

    @pl.when(rounds > 1)
    def _():
        copies = [
            pltpu.make_async_copy(index_hbm, index_ref, index_sem),
            pltpu.make_async_copy(weight_hbm, weight_ref, weight_sem),
            pltpu.make_async_copy(length_hbm, length_ref, length_sem),
        ]
        for copy in copies:
            copy.start()
        for copy in copies:
            copy.wait()
        read_positions(start_ref, index_ref, weight_ref, length_ref, rank_ref, code_ref, rows)

    def later_round(number, inexact):
        fill_slots(rank_ref, code_ref, later_refs, number * slots)
        return spread_half(later_refs, spread_ref, core, tiles, inexact, True)

    inexact = lax.fori_loop(1, rounds, later_round, inexact)
    table_copy.wait()
    multiply(spread_ref, table_ref, inexact, out_ref)


def kernels(table_rows, index_rows, weight, length, row_start, core):
    rows, width = table_rows.shape
    bag, batch = weight.shape
    padded = bag + 8 - bag % 8
    groups = batch * slots // lanes
    half = batch // 2
    tiles = rows // lanes
    smem = pl.BlockSpec(memory_space=pltpu.SMEM)
    vmem = pl.BlockSpec(memory_space=pltpu.VMEM)
    far = pl.BlockSpec(memory_space=pl.ANY)
    table_scratch = pltpu.VMEM((rows, width), table_rows.dtype)
    by_position = [pltpu.VMEM((padded, batch), jnp.float32)] * 2
    by_group = [pltpu.VMEM((groups, lanes), jnp.float32)] * 3
    spread = pltpu.VMEM(((half + 1) * tiles, lanes), jnp.float32)
    dma = pltpu.SemaphoreType.DMA
    pools = jax.ShapeDtypeStruct((half, width), jnp.float32)
    slot = jax.ShapeDtypeStruct((groups, lanes), jnp.float32)
    place = (row_start.reshape(1), core.reshape(1))

    sent, high, low, factor, rounds = pl.pallas_call(
        send_kernel,
        out_shape=(pools, slot, slot, slot, jax.ShapeDtypeStruct((1,), jnp.int32)),
        in_specs=[smem, smem, vmem, vmem, vmem, far],
        out_specs=(vmem, vmem, vmem, vmem, smem),
        scratch_shapes=[table_scratch, *by_position, *by_group, spread, dma],
    )(*place, index_rows, weight, length, table_rows)

    def keep():
        return pl.pallas_call(
            keep_kernel,
            out_shape=pools,
            in_specs=[smem, smem, smem, vmem, vmem, vmem, far, far, far, far],
            out_specs=vmem,
            scratch_shapes=[
                table_scratch,
                pltpu.VMEM(index_rows.shape, index_rows.dtype),
                pltpu.VMEM(weight.shape, weight.dtype),
                pltpu.VMEM(length.shape, length.dtype),
                *by_position,
                *by_group,
                spread,
                dma,
                dma,
                dma,
                dma,
            ],
            cost_estimate=pl.CostEstimate(
                flops=8 * half * rows * width, bytes_accessed=rows * width * 2, transcendentals=0
            ),
        )(*place, rounds, high, low, factor, index_rows, weight, length, table_rows)

    return sent, keep


def on_device(tables, indices, weights, lengths):
    _, row_dev, feature_width = tables.shape
    batch_size = indices.shape[2]
    table_count = lax.axis_size("table")
    pair_count = lax.axis_size("pair")
    core = lax.axis_index("core").astype(jnp.int32)
    row = lax.axis_index("pair").astype(jnp.int32) * 2 + core
    index_rows = indices.transpose(1, 0, 2)
    sent, keep = kernels(tables[0], index_rows, weights[0], lengths, row * row_dev, core)
    received = lax.ppermute(sent, "core", [(0, 1), (1, 0)])
    partial = keep() + received
    share = batch_size // (table_count * pair_count * 2)
    tiles = partial.reshape(table_count * pair_count, share, feature_width)
    arrived = lax.all_to_all(tiles, ("table", "pair"), split_axis=0, concat_axis=0, tiled=True)
    shares = arrived.reshape(table_count, pair_count, share, feature_width)
    return shares.sum(axis=1).astype(jnp.bfloat16)


def solution(mesh):
    tables, rows = mesh.devices.shape
    by_core = Mesh(mesh.devices.reshape(tables, rows // 2, 2), ("table", "pair", "core"))
    row = ("pair", "core")
    placed = (
        P("table", row, None),
        P("table", None, None),
        P("table", None, None),
        P("table", None),
    )
    return jax.shard_map(
        on_device,
        mesh=by_core,
        in_specs=placed,
        out_specs=P(None, ("table", *row), None),
        check_vma=False,
    )
```

```python
import jax
import jax.numpy as jnp
from jax import lax
from jax.experimental import pallas as pl
from jax.experimental.pallas import tpu as pltpu
from jax.sharding import Mesh
from jax.sharding import PartitionSpec as P

lanes = 128
packed_rows = 16
slots = 16
weight_unit = 1024
vmem_bytes = 20 * 2**20


def read_positions(start_ref, index_ref, weight_ref, length_ref, rank_ref, code_ref, rows):
    bag, _, batch = index_ref.shape
    padded = rank_ref.shape[0]
    local = index_ref[:, 0, :] - start_ref[0]
    position = lax.broadcasted_iota(jnp.int32, (bag, batch), 0)
    inside = (local >= 0) & (local < rows) & (position < length_ref[...])
    code = local.astype(jnp.float32) * (2.0 * weight_unit)
    code = code + weight_ref[...].astype(jnp.float32) * weight_unit
    code_ref[:bag, :] = jnp.where(inside, code, 0.0)
    code_ref[bag:, :] = jnp.zeros((padded - bag, batch), jnp.float32)

    used = jnp.where(inside, 1.0, 0.0)
    used = jnp.concatenate([used, jnp.zeros((lanes - bag, batch), jnp.float32)], 0)
    before = lax.broadcasted_iota(jnp.int32, (padded, lanes), 0) > lax.broadcasted_iota(
        jnp.int32, (padded, lanes), 1
    )
    rank = jnp.dot(
        jnp.where(before, 1.0, 0.0).astype(jnp.bfloat16),
        used.astype(jnp.bfloat16),
        preferred_element_type=jnp.float32,
    )
    rank_ref[...] = rank
    return (jnp.max(rank[padded - 1 :, :]).astype(jnp.int32) + (slots - 1)) // slots


def fill_slots(rank_ref, code_ref, slot_refs, first):
    high_ref, low_ref, factor_ref = slot_refs
    groups = high_ref.shape[0]
    planes = []
    for block in range(rank_ref.shape[1] // lanes):
        where = pl.ds(block * lanes, lanes)
        rank = rank_ref[:, where]
        code = code_ref[:, where]
        for s in range(slots):
            at = rank == (first + s).astype(jnp.float32)
            planes.append(jnp.sum(jnp.where(at, code, 0.0), axis=0, keepdims=True))
    plane = jnp.concatenate(planes, 0)
    plane = jnp.concatenate([plane, pltpu.roll(plane, lanes - groups, 1)], 0)
    code = plane.T[:groups].astype(jnp.int32)
    row = code // (2 * weight_unit)
    high_ref[...] = (row // lanes).astype(jnp.float32)
    low_ref[...] = (row % lanes).astype(jnp.float32)
    factor = (code % (2 * weight_unit)).astype(jnp.float32)
    factor_ref[...] = factor * (1.0 / weight_unit)


def spread_half(slot_refs, spread_ref, core, tiles, inexact, add):
    high_ref, low_ref, factor_ref = slot_refs
    group_bags = lanes // slots
    half_groups = high_ref.shape[0] // 2
    stride = spread_ref.shape[0] // tiles
    row_id = lax.broadcasted_iota(jnp.int32, (packed_rows, lanes), 0)
    row_ids = [
        (row_id + packed_rows * i).astype(jnp.float32).astype(jnp.bfloat16)
        for i in range(lanes // packed_rows)
    ]
    zero = jnp.zeros((packed_rows, lanes), jnp.bfloat16)
    one = jnp.ones((packed_rows, lanes), jnp.bfloat16)
    owner = lax.broadcasted_iota(jnp.int32, (packed_rows, lanes), 1) // slots
    owner = owner.astype(jnp.float32).astype(jnp.bfloat16)
    owned = [owner == jnp.full_like(owner, g) for g in range(group_bags)]
    inexact = list(inexact)

    def row_of(ref, j):
        row = ref[pl.ds(j, 1), :]
        return jnp.broadcast_to(row, (packed_rows, lanes)).astype(jnp.bfloat16)

    for t in range(half_groups):
        j = t // 2 * 4 + t % 2 + 2 * core
        high = row_of(high_ref, j)
        low = row_of(low_ref, j)
        factor = row_of(factor_ref, j)
        at = [high == ids for ids in row_ids[: tiles // packed_rows]]
        by_high = []
        for g in range(group_bags):
            mine = jnp.where(owned[g], factor, zero)
            by_high += [jnp.where(hit, mine, zero) for hit in at]
        by_low = [jnp.where(low == ids, one, zero) for ids in row_ids]
        total = lax.dot_general(
            jnp.concatenate(by_high, 0),
            jnp.concatenate(by_low, 0),
            (((1,), (1,)), ((), ())),
            preferred_element_type=jnp.float32,
        )
        blocks = group_bags // 2
        for g in range(group_bags):
            first = (g % blocks * 2 + g // blocks) * half_groups
            where = pl.ds(first + t, tiles, stride=stride)
            part = total[g * tiles : (g + 1) * tiles]
            if add:
                part = part + spread_ref[where, :]
            spread_ref[where, :] = part
            rest = jnp.abs(part - part.astype(jnp.bfloat16).astype(jnp.float32))
            for o in range(len(inexact)):
                inexact[o] = jnp.maximum(inexact[o], rest[o * 8 : (o + 1) * 8])
    return tuple(inexact)


def multiply(spread_ref, table_ref, inexact, out_ref):
    tiles = table_ref.shape[0] // lanes
    stride = spread_ref.shape[0] // tiles
    bags = out_ref.shape[0]
    factors = [
        spread_ref[pl.ds(i * stride, bags), :].astype(jnp.bfloat16) for i in range(tiles)
    ]
    out_ref[...] = jnp.dot(
        jnp.concatenate(factors, 1), table_ref[...], preferred_element_type=jnp.float32
    )

    for o in range(len(inexact)):

        @pl.when(jnp.max(inexact[o]) > 0)
        def _(o=o):
            factors = jnp.concatenate(
                [spread_ref[pl.ds((8 * o + i) * stride, bags), :] for i in range(8)], 1
            )
            rest = factors - factors.astype(jnp.bfloat16).astype(jnp.float32)
            out_ref[...] += jnp.dot(
                rest.astype(jnp.bfloat16),
                table_ref[pl.ds(8 * o * lanes, 8 * lanes), :],
                preferred_element_type=jnp.float32,
            )


def exact_so_far(tiles):
    return tuple(jnp.zeros((8, lanes), jnp.float32) for _ in range(tiles // 8))


def send_kernel(
    start_ref,
    core_ref,
    index_hbm,
    weight_hbm,
    length_hbm,
    table_hbm,
    out_ref,
    high_ref,
    low_ref,
    factor_ref,
    rounds_ref,
    table_ref,
    index_ref,
    weight_ref,
    length_ref,
    rank_ref,
    code_ref,
    high_later,
    low_later,
    factor_later,
    spread_ref,
    table_sem,
    index_sem,
    weight_sem,
    length_sem,
):
    copies = [
        pltpu.make_async_copy(index_hbm, index_ref, index_sem),
        pltpu.make_async_copy(weight_hbm, weight_ref, weight_sem),
        pltpu.make_async_copy(length_hbm, length_ref, length_sem),
    ]
    for copy in copies:
        copy.start()
    table_copy = pltpu.make_async_copy(table_hbm, table_ref, table_sem)
    table_copy.start()
    for copy in copies:
        copy.wait()
    rows = table_ref.shape[0]
    tiles = rows // lanes
    core = 1 - core_ref[0]
    rounds = read_positions(
        start_ref, index_ref, weight_ref, length_ref, rank_ref, code_ref, rows
    )
    rounds_ref[0] = rounds
    slot_refs = (high_ref, low_ref, factor_ref)
    later_refs = (high_later, low_later, factor_later)
    fill_slots(rank_ref, code_ref, slot_refs, jnp.int32(0))
    inexact = spread_half(slot_refs, spread_ref, core, tiles, exact_so_far(tiles), False)

    def later_round(number, inexact):
        fill_slots(rank_ref, code_ref, later_refs, number * slots)
        return spread_half(later_refs, spread_ref, core, tiles, inexact, True)

    inexact = lax.fori_loop(1, rounds, later_round, inexact)
    table_copy.wait()
    multiply(spread_ref, table_ref, inexact, out_ref)


def keep_kernel(
    start_ref,
    core_ref,
    rounds_ref,
    high_ref,
    low_ref,
    factor_ref,
    index_hbm,
    weight_hbm,
    length_hbm,
    table_hbm,
    out_ref,
    table_ref,
    index_ref,
    weight_ref,
    length_ref,
    rank_ref,
    code_ref,
    high_later,
    low_later,
    factor_later,
    spread_ref,
    table_sem,
    index_sem,
    weight_sem,
    length_sem,
):
    table_copy = pltpu.make_async_copy(table_hbm, table_ref, table_sem)
    table_copy.start()
    rows = table_ref.shape[0]
    tiles = rows // lanes
    core = core_ref[0]
    slot_refs = (high_ref, low_ref, factor_ref)
    later_refs = (high_later, low_later, factor_later)
    inexact = spread_half(slot_refs, spread_ref, core, tiles, exact_so_far(tiles), False)
    rounds = rounds_ref[0]

    @pl.when(rounds > 1)
    def _():
        copies = [
            pltpu.make_async_copy(index_hbm, index_ref, index_sem),
            pltpu.make_async_copy(weight_hbm, weight_ref, weight_sem),
            pltpu.make_async_copy(length_hbm, length_ref, length_sem),
        ]
        for copy in copies:
            copy.start()
        for copy in copies:
            copy.wait()
        read_positions(start_ref, index_ref, weight_ref, length_ref, rank_ref, code_ref, rows)

    def later_round(number, inexact):
        fill_slots(rank_ref, code_ref, later_refs, number * slots)
        return spread_half(later_refs, spread_ref, core, tiles, inexact, True)

    inexact = lax.fori_loop(1, rounds, later_round, inexact)
    table_copy.wait()
    multiply(spread_ref, table_ref, inexact, out_ref)


def kernels(table_rows, index_rows, weight, length, row_start, core):
    rows, width = table_rows.shape
    bag, batch = weight.shape
    padded = bag + 8 - bag % 8
    groups = batch * slots // lanes
    half = batch // 2
    tiles = rows // lanes
    smem = pl.BlockSpec(memory_space=pltpu.SMEM)
    vmem = pl.BlockSpec(memory_space=pltpu.VMEM)
    far = pl.BlockSpec(memory_space=pl.ANY)
    table_scratch = pltpu.VMEM((rows, width), table_rows.dtype)
    by_position = [pltpu.VMEM((padded, batch), jnp.float32)] * 2
    by_group = [pltpu.VMEM((groups, lanes), jnp.float32)] * 3
    spread = pltpu.VMEM(((half + 1) * tiles, lanes), jnp.float32)
    dma = pltpu.SemaphoreType.DMA
    scratch = [
        table_scratch,
        pltpu.VMEM(index_rows.shape, index_rows.dtype),
        pltpu.VMEM(weight.shape, weight.dtype),
        pltpu.VMEM(length.shape, length.dtype),
        *by_position,
        *by_group,
        spread,
        dma,
        dma,
        dma,
        dma,
    ]
    limit = pltpu.CompilerParams(vmem_limit_bytes=vmem_bytes)
    index_rows, weight, length, table_rows = [
        pltpu.with_memory_space_constraint(value, pltpu.HBM)
        for value in (index_rows, weight, length, table_rows)
    ]
    pools = jax.ShapeDtypeStruct((half, width), jnp.float32)
    slot = jax.ShapeDtypeStruct((groups, lanes), jnp.float32)
    place = (row_start.reshape(1), core.reshape(1))

    sent, high, low, factor, rounds = pl.pallas_call(
        send_kernel,
        out_shape=(pools, slot, slot, slot, jax.ShapeDtypeStruct((1,), jnp.int32)),
        in_specs=[smem, smem, far, far, far, far],
        out_specs=(vmem, vmem, vmem, vmem, smem),
        scratch_shapes=scratch,
        compiler_params=limit,
    )(*place, index_rows, weight, length, table_rows)

    def keep():
        return pl.pallas_call(
            keep_kernel,
            out_shape=pools,
            in_specs=[smem, smem, smem, vmem, vmem, vmem, far, far, far, far],
            out_specs=vmem,
            scratch_shapes=scratch,
            compiler_params=limit,
            cost_estimate=pl.CostEstimate(
                flops=8 * half * rows * width, bytes_accessed=rows * width * 2, transcendentals=0
            ),
        )(*place, rounds, high, low, factor, index_rows, weight, length, table_rows)

    return sent, keep


def on_device(tables, indices, weights, lengths):
    _, row_dev, feature_width = tables.shape
    batch_size = indices.shape[2]
    table_count = lax.axis_size("table")
    pair_count = lax.axis_size("pair")
    core = lax.axis_index("core").astype(jnp.int32)
    row = lax.axis_index("pair").astype(jnp.int32) * 2 + core
    index_rows = indices.transpose(1, 0, 2)
    sent, keep = kernels(tables[0], index_rows, weights[0], lengths, row * row_dev, core)
    received = lax.ppermute(sent, "core", [(0, 1), (1, 0)])
    partial = keep() + received
    share = batch_size // (table_count * pair_count * 2)
    tiles = partial.reshape(table_count * pair_count, share, feature_width)
    arrived = lax.all_to_all(tiles, ("table", "pair"), split_axis=0, concat_axis=0, tiled=True)
    shares = arrived.reshape(table_count, pair_count, share, feature_width)
    return shares.sum(axis=1).astype(jnp.bfloat16)


def solution(mesh):
    tables, rows = mesh.devices.shape
    by_core = Mesh(mesh.devices.reshape(tables, rows // 2, 2), ("table", "pair", "core"))
    row = ("pair", "core")
    placed = (
        P("table", row, None),
        P("table", None, None),
        P("table", None, None),
        P("table", None),
    )
    return jax.shard_map(
        on_device,
        mesh=by_core,
        in_specs=placed,
        out_specs=P(None, ("table", *row), None),
        check_vma=False,
    )
```

```python
import jax
import jax.numpy as jnp
from jax import lax
from jax.experimental import pallas as pl
from jax.experimental.pallas import tpu as pltpu
from jax.sharding import Mesh
from jax.sharding import PartitionSpec as P

lanes = 128
packed_rows = 16
slots = 16
weight_unit = 1024
vmem_bytes = 20 * 2**20


def read_positions(start_ref, index_ref, weight_ref, length_ref, rank_ref, code_ref, rows):
    bag, _, batch = index_ref.shape
    padded = rank_ref.shape[0]
    local = index_ref[:, 0, :] - start_ref[0]
    position = lax.broadcasted_iota(jnp.int32, (bag, batch), 0)
    inside = (local >= 0) & (local < rows) & (position < length_ref[...])
    code = local.astype(jnp.float32) * (2.0 * weight_unit)
    code = code + weight_ref[...].astype(jnp.float32) * weight_unit
    code_ref[:bag, :] = jnp.where(inside, code, 0.0)
    code_ref[bag:, :] = jnp.zeros((padded - bag, batch), jnp.float32)

    used = jnp.where(inside, 1.0, 0.0)
    used = jnp.concatenate([used, jnp.zeros((lanes - bag, batch), jnp.float32)], 0)
    before = lax.broadcasted_iota(jnp.int32, (padded, lanes), 0) > lax.broadcasted_iota(
        jnp.int32, (padded, lanes), 1
    )
    rank = jnp.dot(
        jnp.where(before, 1.0, 0.0).astype(jnp.bfloat16),
        used.astype(jnp.bfloat16),
        preferred_element_type=jnp.float32,
    )
    rank_ref[...] = rank
    return jnp.max(rank[padded - 1 :, :], keepdims=True)


def rounds_for(most):
    return (jnp.max(most).astype(jnp.int32) + (slots - 1)) // slots


def fill_slots(rank_ref, code_ref, slot_refs, first):
    high_ref, low_ref, factor_ref = slot_refs
    groups = high_ref.shape[0]
    planes = []
    for block in range(rank_ref.shape[1] // lanes):
        where = pl.ds(block * lanes, lanes)
        rank = rank_ref[:, where]
        code = code_ref[:, where]
        for s in range(slots):
            at = rank == (first + s).astype(jnp.float32)
            planes.append(jnp.sum(jnp.where(at, code, 0.0), axis=0, keepdims=True))
    plane = jnp.concatenate(planes, 0)
    plane = jnp.concatenate([plane, pltpu.roll(plane, lanes - groups, 1)], 0)
    code = plane.T[:groups].astype(jnp.int32)
    row = code // (2 * weight_unit)
    high_ref[...] = (row // lanes).astype(jnp.float32)
    low_ref[...] = (row % lanes).astype(jnp.float32)
    factor = (code % (2 * weight_unit)).astype(jnp.float32)
    factor_ref[...] = factor * (1.0 / weight_unit)


def spread_half(slot_refs, spread_ref, core, tiles, inexact, add):
    high_ref, low_ref, factor_ref = slot_refs
    group_bags = lanes // slots
    half_groups = high_ref.shape[0] // 2
    stride = spread_ref.shape[0] // tiles
    row_id = lax.broadcasted_iota(jnp.int32, (packed_rows, lanes), 0)
    row_ids = [
        (row_id + packed_rows * i).astype(jnp.float32).astype(jnp.bfloat16)
        for i in range(lanes // packed_rows)
    ]
    zero = jnp.zeros((packed_rows, lanes), jnp.bfloat16)
    one = jnp.ones((packed_rows, lanes), jnp.bfloat16)
    owner = lax.broadcasted_iota(jnp.int32, (packed_rows, lanes), 1) // slots
    owner = owner.astype(jnp.float32).astype(jnp.bfloat16)
    owned = [owner == jnp.full_like(owner, g) for g in range(group_bags)]
    inexact = list(inexact)

    def row_of(ref, j):
        row = ref[pl.ds(j, 1), :]
        return jnp.broadcast_to(row, (packed_rows, lanes)).astype(jnp.bfloat16)

    for t in range(half_groups):
        j = t // 2 * 4 + t % 2 + 2 * core
        high = row_of(high_ref, j)
        low = row_of(low_ref, j)
        factor = row_of(factor_ref, j)
        at = [high == ids for ids in row_ids[: tiles // packed_rows]]
        by_high = []
        for g in range(group_bags):
            mine = jnp.where(owned[g], factor, zero)
            by_high += [jnp.where(hit, mine, zero) for hit in at]
        by_low = [jnp.where(low == ids, one, zero) for ids in row_ids]
        total = lax.dot_general(
            jnp.concatenate(by_high, 0),
            jnp.concatenate(by_low, 0),
            (((1,), (1,)), ((), ())),
            preferred_element_type=jnp.float32,
        )
        blocks = group_bags // 2
        for g in range(group_bags):
            first = (g % blocks * 2 + g // blocks) * half_groups
            where = pl.ds(first + t, tiles, stride=stride)
            part = total[g * tiles : (g + 1) * tiles]
            if add:
                part = part + spread_ref[where, :]
            spread_ref[where, :] = part
            rest = jnp.abs(part - part.astype(jnp.bfloat16).astype(jnp.float32))
            for o in range(len(inexact)):
                inexact[o] = jnp.maximum(inexact[o], rest[o * 8 : (o + 1) * 8])
    return tuple(inexact)


def multiply(spread_ref, table_ref, inexact, out_ref):
    tiles = table_ref.shape[0] // lanes
    stride = spread_ref.shape[0] // tiles
    bags = out_ref.shape[0]
    left = [jnp.max(most) for most in inexact]
    factors = [
        spread_ref[pl.ds(i * stride, bags), :].astype(jnp.bfloat16) for i in range(tiles)
    ]
    out_ref[...] = jnp.dot(
        jnp.concatenate(factors, 1), table_ref[...], preferred_element_type=jnp.float32
    )

    for o in range(len(inexact)):

        @pl.when(left[o] > 0)
        def _(o=o):
            factors = jnp.concatenate(
                [spread_ref[pl.ds((8 * o + i) * stride, bags), :] for i in range(8)], 1
            )
            rest = factors - factors.astype(jnp.bfloat16).astype(jnp.float32)
            out_ref[...] += jnp.dot(
                rest.astype(jnp.bfloat16),
                table_ref[pl.ds(8 * o * lanes, 8 * lanes), :],
                preferred_element_type=jnp.float32,
            )


def exact_so_far(tiles):
    return tuple(jnp.zeros((8, lanes), jnp.float32) for _ in range(tiles // 8))


def send_kernel(
    start_ref,
    core_ref,
    index_hbm,
    weight_hbm,
    length_hbm,
    table_hbm,
    out_ref,
    high_ref,
    low_ref,
    factor_ref,
    most_ref,
    table_ref,
    index_ref,
    weight_ref,
    length_ref,
    rank_ref,
    code_ref,
    high_later,
    low_later,
    factor_later,
    spread_ref,
    table_sem,
    index_sem,
    weight_sem,
    length_sem,
):
    copies = [
        pltpu.make_async_copy(index_hbm, index_ref, index_sem),
        pltpu.make_async_copy(weight_hbm, weight_ref, weight_sem),
        pltpu.make_async_copy(length_hbm, length_ref, length_sem),
    ]
    for copy in copies:
        copy.start()
    for copy in copies:
        copy.wait()
    table_copy = pltpu.make_async_copy(table_hbm, table_ref, table_sem)
    table_copy.start()
    rows = table_ref.shape[0]
    tiles = rows // lanes
    core = 1 - core_ref[0]
    most = read_positions(
        start_ref, index_ref, weight_ref, length_ref, rank_ref, code_ref, rows
    )
    most_ref[...] = jnp.broadcast_to(most, most_ref.shape)
    rounds = rounds_for(most)
    slot_refs = (high_ref, low_ref, factor_ref)
    later_refs = (high_later, low_later, factor_later)
    fill_slots(rank_ref, code_ref, slot_refs, jnp.int32(0))
    inexact = spread_half(slot_refs, spread_ref, core, tiles, exact_so_far(tiles), False)

    def later_round(number, inexact):
        fill_slots(rank_ref, code_ref, later_refs, number * slots)
        return spread_half(later_refs, spread_ref, core, tiles, inexact, True)

    inexact = lax.fori_loop(1, rounds, later_round, inexact)
    table_copy.wait()
    multiply(spread_ref, table_ref, inexact, out_ref)


def keep_kernel(
    start_ref,
    core_ref,
    most_ref,
    high_ref,
    low_ref,
    factor_ref,
    index_hbm,
    weight_hbm,
    length_hbm,
    table_hbm,
    out_ref,
    table_ref,
    index_ref,
    weight_ref,
    length_ref,
    rank_ref,
    code_ref,
    high_later,
    low_later,
    factor_later,
    spread_ref,
    table_sem,
    index_sem,
    weight_sem,
    length_sem,
):
    table_copy = pltpu.make_async_copy(table_hbm, table_ref, table_sem)
    table_copy.start()
    rows = table_ref.shape[0]
    tiles = rows // lanes
    core = core_ref[0]
    slot_refs = (high_ref, low_ref, factor_ref)
    later_refs = (high_later, low_later, factor_later)
    inexact = spread_half(slot_refs, spread_ref, core, tiles, exact_so_far(tiles), False)
    rounds = rounds_for(most_ref[...])

    @pl.when(rounds > 1)
    def _():
        copies = [
            pltpu.make_async_copy(index_hbm, index_ref, index_sem),
            pltpu.make_async_copy(weight_hbm, weight_ref, weight_sem),
            pltpu.make_async_copy(length_hbm, length_ref, length_sem),
        ]
        for copy in copies:
            copy.start()
        for copy in copies:
            copy.wait()
        read_positions(start_ref, index_ref, weight_ref, length_ref, rank_ref, code_ref, rows)

    def later_round(number, inexact):
        fill_slots(rank_ref, code_ref, later_refs, number * slots)
        return spread_half(later_refs, spread_ref, core, tiles, inexact, True)

    inexact = lax.fori_loop(1, rounds, later_round, inexact)
    table_copy.wait()
    multiply(spread_ref, table_ref, inexact, out_ref)


def kernels(table_rows, index_rows, weight, length, row_start, core):
    rows, width = table_rows.shape
    bag, batch = weight.shape
    padded = bag + 8 - bag % 8
    groups = batch * slots // lanes
    half = batch // 2
    tiles = rows // lanes
    smem = pl.BlockSpec(memory_space=pltpu.SMEM)
    vmem = pl.BlockSpec(memory_space=pltpu.VMEM)
    far = pl.BlockSpec(memory_space=pl.ANY)
    table_scratch = pltpu.VMEM((rows, width), table_rows.dtype)
    by_position = [pltpu.VMEM((padded, batch), jnp.float32)] * 2
    by_group = [pltpu.VMEM((groups, lanes), jnp.float32)] * 3
    spread = pltpu.VMEM(((half + 1) * tiles, lanes), jnp.float32)
    dma = pltpu.SemaphoreType.DMA
    scratch = [
        table_scratch,
        pltpu.VMEM(index_rows.shape, index_rows.dtype),
        pltpu.VMEM(weight.shape, weight.dtype),
        pltpu.VMEM(length.shape, length.dtype),
        *by_position,
        *by_group,
        spread,
        dma,
        dma,
        dma,
        dma,
    ]
    limit = pltpu.CompilerParams(vmem_limit_bytes=vmem_bytes)
    index_rows, weight, length, table_rows = [
        pltpu.with_memory_space_constraint(value, pltpu.HBM)
        for value in (index_rows, weight, length, table_rows)
    ]
    pools = jax.ShapeDtypeStruct((half, width), jnp.float32)
    slot = jax.ShapeDtypeStruct((groups, lanes), jnp.float32)
    place = (row_start.reshape(1), core.reshape(1))

    sent, high, low, factor, most = pl.pallas_call(
        send_kernel,
        out_shape=(pools, slot, slot, slot, jax.ShapeDtypeStruct((8, lanes), jnp.float32)),
        in_specs=[smem, smem, far, far, far, far],
        out_specs=(vmem, vmem, vmem, vmem, vmem),
        scratch_shapes=scratch,
        compiler_params=limit,
    )(*place, index_rows, weight, length, table_rows)

    def keep():
        return pl.pallas_call(
            keep_kernel,
            out_shape=pools,
            in_specs=[smem, smem, vmem, vmem, vmem, vmem, far, far, far, far],
            out_specs=vmem,
            scratch_shapes=scratch,
            compiler_params=limit,
            cost_estimate=pl.CostEstimate(
                flops=8 * half * rows * width, bytes_accessed=rows * width * 2, transcendentals=0
            ),
        )(*place, most, high, low, factor, index_rows, weight, length, table_rows)

    return sent, keep


def on_device(tables, indices, weights, lengths):
    _, row_dev, feature_width = tables.shape
    batch_size = indices.shape[2]
    table_count = lax.axis_size("table")
    pair_count = lax.axis_size("pair")
    core = lax.axis_index("core").astype(jnp.int32)
    row = lax.axis_index("pair").astype(jnp.int32) * 2 + core
    index_rows = indices.transpose(1, 0, 2)
    sent, keep = kernels(tables[0], index_rows, weights[0], lengths, row * row_dev, core)
    received = lax.ppermute(sent, "core", [(0, 1), (1, 0)])
    partial = keep() + received
    share = batch_size // (table_count * pair_count * 2)
    tiles = partial.reshape(table_count * pair_count, share, feature_width)
    arrived = lax.all_to_all(tiles, ("table", "pair"), split_axis=0, concat_axis=0, tiled=True)
    shares = arrived.reshape(table_count, pair_count, share, feature_width)
    return shares.sum(axis=1).astype(jnp.bfloat16)


def solution(mesh):
    tables, rows = mesh.devices.shape
    by_core = Mesh(mesh.devices.reshape(tables, rows // 2, 2), ("table", "pair", "core"))
    row = ("pair", "core")
    placed = (
        P("table", row, None),
        P("table", None, None),
        P("table", None, None),
        P("table", None),
    )
    return jax.shard_map(
        on_device,
        mesh=by_core,
        in_specs=placed,
        out_specs=P(None, ("table", *row), None),
        check_vma=False,
    )
```

```python
import functools

import jax
import jax.numpy as jnp
from jax import lax
from jax.experimental import pallas as pl
from jax.experimental.pallas import tpu as pltpu
from jax.sharding import Mesh
from jax.sharding import PartitionSpec as P

lanes = 128
packed_rows = 16
slots = 16
weight_unit = 1024
vmem_bytes = 20 * 2**20


def read_positions(start_ref, index_ref, weight_ref, length_ref, rank_ref, code_ref, rows):
    bag, _, batch = index_ref.shape
    padded = rank_ref.shape[0]
    local = index_ref[:, 0, :] - start_ref[0]
    position = lax.broadcasted_iota(jnp.int32, (bag, batch), 0)
    inside = (local >= 0) & (local < rows) & (position < length_ref[...])
    code = local.astype(jnp.float32) * (2.0 * weight_unit)
    code = code + weight_ref[...].astype(jnp.float32) * weight_unit
    code_ref[:bag, :] = jnp.where(inside, code, 0.0)
    code_ref[bag:, :] = jnp.zeros((padded - bag, batch), jnp.float32)

    used = jnp.where(inside, 1.0, 0.0)
    used = jnp.concatenate([used, jnp.zeros((lanes - bag, batch), jnp.float32)], 0)
    before = lax.broadcasted_iota(jnp.int32, (padded, lanes), 0) > lax.broadcasted_iota(
        jnp.int32, (padded, lanes), 1
    )
    rank = jnp.dot(
        jnp.where(before, 1.0, 0.0).astype(jnp.bfloat16),
        used.astype(jnp.bfloat16),
        preferred_element_type=jnp.float32,
    )
    rank_ref[...] = rank
    return jnp.max(rank[padded - 1 :, :], keepdims=True)


def rounds_for(most):
    return (jnp.max(most).astype(jnp.int32) + (slots - 1)) // slots


def note_repeats(plane, repeated_ref):
    row = (plane.astype(jnp.int32) // (2 * weight_unit)).astype(jnp.float32)
    slot = lax.broadcasted_iota(jnp.int32, plane.shape, 0).astype(jnp.float32)
    row = jnp.where(plane > 0, row, -1.0 - slot)
    noted = []
    for first in range(0, plane.shape[0], slots):
        rows = row[first : first + slots]
        again = jnp.full(rows.shape, -1.0, jnp.float32)
        for shift in range(1, slots // 2 + 1):
            again = jnp.where(rows == pltpu.roll(rows, shift, 0), rows, again)
        noted.append((again.astype(jnp.int32) >> 8).astype(jnp.float32))
    for pair in range(repeated_ref.shape[0]):
        hits = functools.reduce(
            jnp.maximum, [jnp.where(pairs == float(pair), 1.0, 0.0) for pairs in noted]
        )
        repeated_ref[pair : pair + 1, :] = jnp.max(hits, axis=0, keepdims=True)


def fill_slots(rank_ref, code_ref, slot_refs, first, repeated_ref=None):
    high_ref, low_ref, factor_ref = slot_refs
    groups = high_ref.shape[0]
    planes = []
    for block in range(rank_ref.shape[1] // lanes):
        where = pl.ds(block * lanes, lanes)
        rank = rank_ref[:, where]
        code = code_ref[:, where]
        for s in range(slots):
            at = rank == (first + s).astype(jnp.float32)
            planes.append(jnp.sum(jnp.where(at, code, 0.0), axis=0, keepdims=True))
    plane = jnp.concatenate(planes, 0)
    if repeated_ref is not None:
        note_repeats(plane, repeated_ref)
    plane = jnp.concatenate([plane, pltpu.roll(plane, lanes - groups, 1)], 0)
    low_ref[...] = (plane.astype(jnp.int32) // (2 * weight_unit) % lanes).astype(jnp.float32)
    code = plane.T[:groups].astype(jnp.int32)
    row = code // (2 * weight_unit)
    high_ref[...] = (row // lanes).astype(jnp.float32)
    factor = (code % (2 * weight_unit)).astype(jnp.float32)
    factor_ref[...] = factor * (1.0 / weight_unit)


def spread_half(slot_refs, spread_ref, core, tiles, add):
    high_ref, low_ref, factor_ref = slot_refs
    group_bags = lanes // slots
    half_groups = high_ref.shape[0] // 2
    stride = spread_ref.shape[0] // tiles
    row_id = lax.broadcasted_iota(jnp.int32, (packed_rows, lanes), 0)
    row_ids = [
        (row_id + packed_rows * i).astype(jnp.float32).astype(jnp.bfloat16)
        for i in range(tiles // packed_rows)
    ]
    zero = jnp.zeros((packed_rows, lanes), jnp.bfloat16)
    lane = lax.broadcasted_iota(jnp.int32, (lanes, lanes), 1).astype(jnp.float32)
    lows = pltpu.roll(low_ref[...], (lanes - 2 * core) % lanes, 1)
    owner = lax.broadcasted_iota(jnp.int32, (packed_rows, lanes), 1) // slots
    owner = owner.astype(jnp.float32).astype(jnp.bfloat16)
    owned = [owner == jnp.full_like(owner, g) for g in range(group_bags)]

    def row_of(ref, j):
        row = ref[pl.ds(j, 1), :]
        return jnp.broadcast_to(row, (packed_rows, lanes)).astype(jnp.bfloat16)

    for t in range(half_groups):
        j = t // 2 * 4 + t % 2 + 2 * core
        high = row_of(high_ref, j)
        factor = row_of(factor_ref, j)
        at = [high == ids for ids in row_ids]
        by_high = []
        for g in range(group_bags):
            mine = jnp.where(owned[g], factor, zero)
            by_high += [jnp.where(hit, mine, zero) for hit in at]
        at_lane = t // 2 * 4 + t % 2
        low = jnp.broadcast_to(lows[:, at_lane : at_lane + 1], (lanes, lanes))
        by_low = jnp.where(low == lane, 1.0, 0.0).astype(jnp.bfloat16)
        total = lax.dot_general(
            jnp.concatenate(by_high, 0),
            by_low,
            (((1,), (0,)), ((), ())),
            preferred_element_type=jnp.float32,
        )
        blocks = group_bags // 2
        for g in range(group_bags):
            first = (g % blocks * 2 + g // blocks) * half_groups
            where = pl.ds(first + t, tiles, stride=stride)
            part = total[g * tiles : (g + 1) * tiles]
            if add:
                part = part + spread_ref[where, :]
            spread_ref[where, :] = part


def multiply(spread_ref, table_ref, repeated_ref, core, rounds, out_ref):
    tiles = table_ref.shape[0] // lanes
    stride = spread_ref.shape[0] // tiles
    bags = out_ref.shape[0]
    lane = lax.broadcasted_iota(jnp.int32, (1, lanes), 1)
    ours = (lane // 2) % 2 == core
    left = [
        jnp.where(ours, repeated_ref[pair : pair + 1, :], 0.0) for pair in range(tiles // 2)
    ]
    any_left = (jnp.max(functools.reduce(jnp.maximum, left)) > 0) | (rounds > 1)
    left = [(jnp.max(some) > 0) | (rounds > 1) for some in left]
    factors = [
        spread_ref[pl.ds(i * stride, bags), :].astype(jnp.bfloat16) for i in range(tiles)
    ]
    out_ref[...] = jnp.dot(
        jnp.concatenate(factors, 1), table_ref[...], preferred_element_type=jnp.float32
    )

    def add_rest(pair):
        factors = [spread_ref[pl.ds((2 * pair + i) * stride, bags), :] for i in range(2)]
        factors = jnp.concatenate(factors, 1)
        rest = factors - factors.astype(jnp.bfloat16).astype(jnp.float32)
        out_ref[...] += jnp.dot(
            rest.astype(jnp.bfloat16),
            table_ref[pl.ds(2 * pair * lanes, 2 * lanes), :],
            preferred_element_type=jnp.float32,
        )

    @pl.when(any_left)
    def _():
        for pair in range(tiles // 2):
            pl.when(left[pair])(functools.partial(add_rest, pair))


def send_kernel(
    start_ref,
    core_ref,
    index_hbm,
    weight_hbm,
    length_hbm,
    table_hbm,
    out_ref,
    high_ref,
    low_ref,
    factor_ref,
    most_ref,
    repeated_ref,
    table_ref,
    index_ref,
    weight_ref,
    length_ref,
    rank_ref,
    code_ref,
    high_later,
    low_later,
    factor_later,
    spread_ref,
    table_sem,
    index_sem,
    weight_sem,
    length_sem,
):
    copies = [
        pltpu.make_async_copy(index_hbm, index_ref, index_sem),
        pltpu.make_async_copy(weight_hbm, weight_ref, weight_sem),
        pltpu.make_async_copy(length_hbm, length_ref, length_sem),
    ]
    for copy in copies:
        copy.start()
    for copy in copies:
        copy.wait()
    table_copy = pltpu.make_async_copy(table_hbm, table_ref, table_sem)
    table_copy.start()
    rows = table_ref.shape[0]
    tiles = rows // lanes
    core = 1 - core_ref[0]
    most = read_positions(
        start_ref, index_ref, weight_ref, length_ref, rank_ref, code_ref, rows
    )
    most_ref[...] = jnp.broadcast_to(most, most_ref.shape)
    rounds = rounds_for(most)
    slot_refs = (high_ref, low_ref, factor_ref)
    later_refs = (high_later, low_later, factor_later)
    fill_slots(rank_ref, code_ref, slot_refs, jnp.int32(0), repeated_ref)
    spread_half(slot_refs, spread_ref, core, tiles, False)

    def later_round(number, carry):
        fill_slots(rank_ref, code_ref, later_refs, number * slots)
        spread_half(later_refs, spread_ref, core, tiles, True)
        return carry

    lax.fori_loop(1, rounds, later_round, 0)
    table_copy.wait()
    multiply(spread_ref, table_ref, repeated_ref, core, rounds, out_ref)


def keep_kernel(
    start_ref,
    core_ref,
    most_ref,
    repeated_ref,
    high_ref,
    low_ref,
    factor_ref,
    index_hbm,
    weight_hbm,
    length_hbm,
    table_hbm,
    out_ref,
    table_ref,
    index_ref,
    weight_ref,
    length_ref,
    rank_ref,
    code_ref,
    high_later,
    low_later,
    factor_later,
    spread_ref,
    table_sem,
    index_sem,
    weight_sem,
    length_sem,
):
    table_copy = pltpu.make_async_copy(table_hbm, table_ref, table_sem)
    table_copy.start()
    rows = table_ref.shape[0]
    tiles = rows // lanes
    core = core_ref[0]
    slot_refs = (high_ref, low_ref, factor_ref)
    later_refs = (high_later, low_later, factor_later)
    spread_half(slot_refs, spread_ref, core, tiles, False)
    rounds = rounds_for(most_ref[...])

    @pl.when(rounds > 1)
    def _():
        copies = [
            pltpu.make_async_copy(index_hbm, index_ref, index_sem),
            pltpu.make_async_copy(weight_hbm, weight_ref, weight_sem),
            pltpu.make_async_copy(length_hbm, length_ref, length_sem),
        ]
        for copy in copies:
            copy.start()
        for copy in copies:
            copy.wait()
        read_positions(start_ref, index_ref, weight_ref, length_ref, rank_ref, code_ref, rows)

    def later_round(number, carry):
        fill_slots(rank_ref, code_ref, later_refs, number * slots)
        spread_half(later_refs, spread_ref, core, tiles, True)
        return carry

    lax.fori_loop(1, rounds, later_round, 0)
    table_copy.wait()
    multiply(spread_ref, table_ref, repeated_ref, core, rounds, out_ref)


def kernels(table_rows, index_rows, weight, length, row_start, core):
    rows, width = table_rows.shape
    bag, batch = weight.shape
    padded = bag + 8 - bag % 8
    groups = batch * slots // lanes
    half = batch // 2
    tiles = rows // lanes
    smem = pl.BlockSpec(memory_space=pltpu.SMEM)
    vmem = pl.BlockSpec(memory_space=pltpu.VMEM)
    far = pl.BlockSpec(memory_space=pl.ANY)
    table_scratch = pltpu.VMEM((rows, width), table_rows.dtype)
    by_position = [pltpu.VMEM((padded, batch), jnp.float32)] * 2
    by_group = [pltpu.VMEM((n, lanes), jnp.float32) for n in (groups, lanes, groups)]
    spread = pltpu.VMEM(((half + 1) * tiles, lanes), jnp.float32)
    dma = pltpu.SemaphoreType.DMA
    scratch = [
        table_scratch,
        pltpu.VMEM(index_rows.shape, index_rows.dtype),
        pltpu.VMEM(weight.shape, weight.dtype),
        pltpu.VMEM(length.shape, length.dtype),
        *by_position,
        *by_group,
        spread,
        dma,
        dma,
        dma,
        dma,
    ]
    limit = pltpu.CompilerParams(vmem_limit_bytes=vmem_bytes)
    index_rows, weight, length, table_rows = [
        pltpu.with_memory_space_constraint(value, pltpu.HBM)
        for value in (index_rows, weight, length, table_rows)
    ]
    pools = jax.ShapeDtypeStruct((half, width), jnp.float32)
    slot = [jax.ShapeDtypeStruct((n, lanes), jnp.float32) for n in (groups, lanes, groups)]
    place = (row_start.reshape(1), core.reshape(1))

    sent, high, low, factor, most, repeated = pl.pallas_call(
        send_kernel,
        out_shape=(
            pools,
            *slot,
            jax.ShapeDtypeStruct((8, lanes), jnp.float32),
            jax.ShapeDtypeStruct((tiles // 2, lanes), jnp.float32),
        ),
        in_specs=[smem, smem, far, far, far, far],
        out_specs=(vmem,) * 6,
        scratch_shapes=scratch,
        compiler_params=limit,
    )(*place, index_rows, weight, length, table_rows)

    def keep():
        return pl.pallas_call(
            keep_kernel,
            out_shape=pools,
            in_specs=[smem, smem, vmem, vmem, vmem, vmem, vmem, far, far, far, far],
            out_specs=vmem,
            scratch_shapes=scratch,
            compiler_params=limit,
            cost_estimate=pl.CostEstimate(
                flops=8 * half * rows * width, bytes_accessed=rows * width * 2, transcendentals=0
            ),
        )(*place, most, repeated, high, low, factor, index_rows, weight, length, table_rows)

    return sent, keep


def on_device(tables, indices, weights, lengths):
    _, row_dev, feature_width = tables.shape
    batch_size = indices.shape[2]
    table_count = lax.axis_size("table")
    pair_count = lax.axis_size("pair")
    core = lax.axis_index("core").astype(jnp.int32)
    row = lax.axis_index("pair").astype(jnp.int32) * 2 + core
    index_rows = indices.transpose(1, 0, 2)
    sent, keep = kernels(tables[0], index_rows, weights[0], lengths, row * row_dev, core)
    received = lax.ppermute(sent, "core", [(0, 1), (1, 0)])
    partial = keep() + received
    share = batch_size // (table_count * pair_count * 2)
    tiles = partial.reshape(table_count * pair_count, share, feature_width)
    arrived = lax.all_to_all(tiles, ("table", "pair"), split_axis=0, concat_axis=0, tiled=True)
    shares = arrived.reshape(table_count, pair_count, share, feature_width)
    return shares.sum(axis=1).astype(jnp.bfloat16)


def solution(mesh):
    tables, rows = mesh.devices.shape
    by_core = Mesh(mesh.devices.reshape(tables, rows // 2, 2), ("table", "pair", "core"))
    row = ("pair", "core")
    placed = (
        P("table", row, None),
        P("table", None, None),
        P("table", None, None),
        P("table", None),
    )
    return jax.shard_map(
        on_device,
        mesh=by_core,
        in_specs=placed,
        out_specs=P(None, ("table", *row), None),
        check_vma=False,
    )
```

```python
import functools

import jax
import jax.numpy as jnp
from jax import lax
from jax.experimental import pallas as pl
from jax.experimental.pallas import tpu as pltpu
from jax.sharding import Mesh
from jax.sharding import PartitionSpec as P

lanes = 128
packed_rows = 16
slots = 16
weight_unit = 1024
far_pair = 26
vmem_bytes = 20 * 2**20


def read_positions(start_ref, index_ref, weight_ref, length_ref, rank_ref, code_ref, rows):
    bag, _, batch = index_ref.shape
    padded = rank_ref.shape[0]
    local = index_ref[:, 0, :] - start_ref[0]
    position = lax.broadcasted_iota(jnp.int32, (bag, batch), 0)
    inside = (local >= 0) & (local < rows) & (position < length_ref[...])
    code = local.astype(jnp.float32) * (2.0 * weight_unit)
    code = code + weight_ref[...].astype(jnp.float32) * weight_unit
    code_ref[:bag, :] = jnp.where(inside, code, 0.0)
    code_ref[bag:, :] = jnp.zeros((padded - bag, batch), jnp.float32)

    used = jnp.where(inside, 1.0, 0.0)
    used = jnp.concatenate([used, jnp.zeros((lanes - bag, batch), jnp.float32)], 0)
    before = lax.broadcasted_iota(jnp.int32, (padded, lanes), 0) > lax.broadcasted_iota(
        jnp.int32, (padded, lanes), 1
    )
    rank = jnp.dot(
        jnp.where(before, 1.0, 0.0).astype(jnp.bfloat16),
        used.astype(jnp.bfloat16),
        preferred_element_type=jnp.float32,
    )
    rank_ref[...] = rank
    return jnp.max(rank[padded - 1 :, :], keepdims=True)


def rounds_for(most):
    return (jnp.max(most).astype(jnp.int32) + (slots - 1)) // slots


def note_repeats(plane, repeated_ref):
    row = (plane.astype(jnp.int32) // (2 * weight_unit)).astype(jnp.float32)
    slot = lax.broadcasted_iota(jnp.int32, plane.shape, 0).astype(jnp.float32)
    row = jnp.where(plane > 0, row, -1.0 - slot)
    noted = []
    for first in range(0, plane.shape[0], slots):
        rows = row[first : first + slots]
        again = jnp.full(rows.shape, -1.0, jnp.float32)
        for shift in range(1, slots // 2 + 1):
            again = jnp.where(rows == pltpu.roll(rows, shift, 0), rows, again)
        noted.append((again.astype(jnp.int32) >> 8).astype(jnp.float32))
    for pair in range(repeated_ref.shape[0]):
        hits = functools.reduce(
            jnp.maximum, [jnp.where(pairs == float(pair), 1.0, 0.0) for pairs in noted]
        )
        repeated_ref[pair : pair + 1, :] = jnp.max(hits, axis=0, keepdims=True)


def fill_slots(rank_ref, code_ref, slot_refs, first, repeated_ref=None):
    high_ref, low_ref, factor_ref = slot_refs
    groups = high_ref.shape[0]
    planes = []
    for block in range(rank_ref.shape[1] // lanes):
        where = pl.ds(block * lanes, lanes)
        rank = rank_ref[:, where]
        code = code_ref[:, where]
        for s in range(slots):
            at = rank == (first + s).astype(jnp.float32)
            planes.append(jnp.sum(jnp.where(at, code, 0.0), axis=0, keepdims=True))
    plane = jnp.concatenate(planes, 0)
    if repeated_ref is not None:
        note_repeats(plane, repeated_ref)
    plane = jnp.concatenate([plane, pltpu.roll(plane, lanes - groups, 1)], 0)
    low_ref[...] = (plane.astype(jnp.int32) // (2 * weight_unit) % lanes).astype(jnp.float32)
    code = plane.T[:groups].astype(jnp.int32)
    row = code // (2 * weight_unit)
    high_ref[...] = (row // lanes).astype(jnp.float32)
    factor = (code % (2 * weight_unit)).astype(jnp.float32)
    factor_ref[...] = factor * (1.0 / weight_unit)


def spread_half(slot_refs, spread_ref, core, tiles, add):
    high_ref, low_ref, factor_ref = slot_refs
    group_bags = lanes // slots
    half_groups = high_ref.shape[0] // 2
    stride = spread_ref.shape[0] // tiles
    row_id = lax.broadcasted_iota(jnp.int32, (packed_rows, lanes), 0)
    row_ids = [
        (row_id + packed_rows * i).astype(jnp.float32).astype(jnp.bfloat16)
        for i in range(tiles // packed_rows)
    ]
    zero = jnp.zeros((packed_rows, lanes), jnp.bfloat16)
    lane = lax.broadcasted_iota(jnp.int32, (lanes, lanes), 1).astype(jnp.float32)
    lows = pltpu.roll(low_ref[...], (lanes - 2 * core) % lanes, 1)
    owner = lax.broadcasted_iota(jnp.int32, (packed_rows, lanes), 1) // slots
    owner = owner.astype(jnp.float32).astype(jnp.bfloat16)
    owned = [owner == jnp.full_like(owner, g) for g in range(group_bags)]

    def row_of(ref, j):
        row = ref[pl.ds(j, 1), :]
        return jnp.broadcast_to(row, (packed_rows, lanes)).astype(jnp.bfloat16)

    for t in range(half_groups):
        j = t // 2 * 4 + t % 2 + 2 * core
        high = row_of(high_ref, j)
        factor = row_of(factor_ref, j)
        at = [high == ids for ids in row_ids]
        by_high = []
        for g in range(group_bags):
            mine = jnp.where(owned[g], factor, zero)
            by_high += [jnp.where(hit, mine, zero) for hit in at]
        at_lane = t // 2 * 4 + t % 2
        low = jnp.broadcast_to(lows[:, at_lane : at_lane + 1], (lanes, lanes))
        by_low = jnp.where(low == lane, 1.0, 0.0).astype(jnp.bfloat16)
        total = lax.dot_general(
            jnp.concatenate(by_high, 0),
            by_low,
            (((1,), (0,)), ((), ())),
            preferred_element_type=jnp.float32,
        )
        blocks = group_bags // 2
        for g in range(group_bags):
            pair = (g // blocks * half_groups + t) // 2 ^ far_pair
            bag = g % blocks * 2 * half_groups + pair * 2 + t % 2
            where = pl.ds(bag, tiles, stride=stride)
            part = total[g * tiles : (g + 1) * tiles]
            if add:
                part = part + spread_ref[where, :]
            spread_ref[where, :] = part


def multiply(spread_ref, table_ref, repeated_ref, core, rounds, out_ref):
    tiles = table_ref.shape[0] // lanes
    stride = spread_ref.shape[0] // tiles
    bags = out_ref.shape[0]
    lane = lax.broadcasted_iota(jnp.int32, (1, lanes), 1)
    ours = (lane // 2) % 2 == core
    left = [
        jnp.where(ours, repeated_ref[pair : pair + 1, :], 0.0) for pair in range(tiles // 2)
    ]
    any_left = (jnp.max(functools.reduce(jnp.maximum, left)) > 0) | (rounds > 1)
    left = [(jnp.max(some) > 0) | (rounds > 1) for some in left]
    factors = [
        spread_ref[pl.ds(i * stride, bags), :].astype(jnp.bfloat16) for i in range(tiles)
    ]
    out_ref[...] = jnp.dot(
        jnp.concatenate(factors, 1), table_ref[...], preferred_element_type=jnp.float32
    )

    def add_rest(pair):
        factors = [spread_ref[pl.ds((2 * pair + i) * stride, bags), :] for i in range(2)]
        factors = jnp.concatenate(factors, 1)
        rest = factors - factors.astype(jnp.bfloat16).astype(jnp.float32)
        out_ref[...] += jnp.dot(
            rest.astype(jnp.bfloat16),
            table_ref[pl.ds(2 * pair * lanes, 2 * lanes), :],
            preferred_element_type=jnp.float32,
        )

    @pl.when(any_left)
    def _():
        for pair in range(tiles // 2):
            pl.when(left[pair])(functools.partial(add_rest, pair))


def send_kernel(
    start_ref,
    core_ref,
    index_hbm,
    weight_hbm,
    length_hbm,
    table_hbm,
    out_ref,
    high_ref,
    low_ref,
    factor_ref,
    most_ref,
    repeated_ref,
    table_ref,
    index_ref,
    weight_ref,
    length_ref,
    rank_ref,
    code_ref,
    high_later,
    low_later,
    factor_later,
    spread_ref,
    table_sem,
    index_sem,
    weight_sem,
    length_sem,
):
    copies = [
        pltpu.make_async_copy(index_hbm, index_ref, index_sem),
        pltpu.make_async_copy(weight_hbm, weight_ref, weight_sem),
        pltpu.make_async_copy(length_hbm, length_ref, length_sem),
    ]
    for copy in copies:
        copy.start()
    for copy in copies:
        copy.wait()
    table_copy = pltpu.make_async_copy(table_hbm, table_ref, table_sem)
    table_copy.start()
    rows = table_ref.shape[0]
    tiles = rows // lanes
    core = 1 - core_ref[0]
    most = read_positions(
        start_ref, index_ref, weight_ref, length_ref, rank_ref, code_ref, rows
    )
    most_ref[...] = jnp.broadcast_to(most, most_ref.shape)
    rounds = rounds_for(most)
    slot_refs = (high_ref, low_ref, factor_ref)
    later_refs = (high_later, low_later, factor_later)
    fill_slots(rank_ref, code_ref, slot_refs, jnp.int32(0), repeated_ref)
    spread_half(slot_refs, spread_ref, core, tiles, False)

    def later_round(number, carry):
        fill_slots(rank_ref, code_ref, later_refs, number * slots)
        spread_half(later_refs, spread_ref, core, tiles, True)
        return carry

    lax.fori_loop(1, rounds, later_round, 0)
    table_copy.wait()
    multiply(spread_ref, table_ref, repeated_ref, core, rounds, out_ref)


def keep_kernel(
    start_ref,
    core_ref,
    most_ref,
    repeated_ref,
    high_ref,
    low_ref,
    factor_ref,
    index_hbm,
    weight_hbm,
    length_hbm,
    table_hbm,
    out_ref,
    table_ref,
    index_ref,
    weight_ref,
    length_ref,
    rank_ref,
    code_ref,
    high_later,
    low_later,
    factor_later,
    spread_ref,
    table_sem,
    index_sem,
    weight_sem,
    length_sem,
):
    table_copy = pltpu.make_async_copy(table_hbm, table_ref, table_sem)
    table_copy.start()
    rows = table_ref.shape[0]
    tiles = rows // lanes
    core = core_ref[0]
    slot_refs = (high_ref, low_ref, factor_ref)
    later_refs = (high_later, low_later, factor_later)
    spread_half(slot_refs, spread_ref, core, tiles, False)
    rounds = rounds_for(most_ref[...])

    @pl.when(rounds > 1)
    def _():
        copies = [
            pltpu.make_async_copy(index_hbm, index_ref, index_sem),
            pltpu.make_async_copy(weight_hbm, weight_ref, weight_sem),
            pltpu.make_async_copy(length_hbm, length_ref, length_sem),
        ]
        for copy in copies:
            copy.start()
        for copy in copies:
            copy.wait()
        read_positions(start_ref, index_ref, weight_ref, length_ref, rank_ref, code_ref, rows)

    def later_round(number, carry):
        fill_slots(rank_ref, code_ref, later_refs, number * slots)
        spread_half(later_refs, spread_ref, core, tiles, True)
        return carry

    lax.fori_loop(1, rounds, later_round, 0)
    table_copy.wait()
    multiply(spread_ref, table_ref, repeated_ref, core, rounds, out_ref)


def kernels(table_rows, index_rows, weight, length, row_start, core):
    rows, width = table_rows.shape
    bag, batch = weight.shape
    padded = bag + 8 - bag % 8
    groups = batch * slots // lanes
    half = batch // 2
    tiles = rows // lanes
    smem = pl.BlockSpec(memory_space=pltpu.SMEM)
    vmem = pl.BlockSpec(memory_space=pltpu.VMEM)
    far = pl.BlockSpec(memory_space=pl.ANY)
    table_scratch = pltpu.VMEM((rows, width), table_rows.dtype)
    by_position = [pltpu.VMEM((padded, batch), jnp.float32)] * 2
    by_group = [pltpu.VMEM((n, lanes), jnp.float32) for n in (groups, lanes, groups)]
    spread = pltpu.VMEM(((half + 1) * tiles, lanes), jnp.float32)
    dma = pltpu.SemaphoreType.DMA
    scratch = [
        table_scratch,
        pltpu.VMEM(index_rows.shape, index_rows.dtype),
        pltpu.VMEM(weight.shape, weight.dtype),
        pltpu.VMEM(length.shape, length.dtype),
        *by_position,
        *by_group,
        spread,
        dma,
        dma,
        dma,
        dma,
    ]
    limit = pltpu.CompilerParams(vmem_limit_bytes=vmem_bytes)
    index_rows, weight, length, table_rows = [
        pltpu.with_memory_space_constraint(value, pltpu.HBM)
        for value in (index_rows, weight, length, table_rows)
    ]
    pools = jax.ShapeDtypeStruct((half, width), jnp.float32)
    slot = [jax.ShapeDtypeStruct((n, lanes), jnp.float32) for n in (groups, lanes, groups)]
    place = (row_start.reshape(1), core.reshape(1))

    sent, high, low, factor, most, repeated = pl.pallas_call(
        send_kernel,
        out_shape=(
            pools,
            *slot,
            jax.ShapeDtypeStruct((8, lanes), jnp.float32),
            jax.ShapeDtypeStruct((tiles // 2, lanes), jnp.float32),
        ),
        in_specs=[smem, smem, far, far, far, far],
        out_specs=(vmem,) * 6,
        scratch_shapes=scratch,
        compiler_params=limit,
    )(*place, index_rows, weight, length, table_rows)

    def keep():
        return pl.pallas_call(
            keep_kernel,
            out_shape=pools,
            in_specs=[smem, smem, vmem, vmem, vmem, vmem, vmem, far, far, far, far],
            out_specs=vmem,
            scratch_shapes=scratch,
            compiler_params=limit,
            cost_estimate=pl.CostEstimate(
                flops=8 * half * rows * width, bytes_accessed=rows * width * 2, transcendentals=0
            ),
        )(*place, most, repeated, high, low, factor, index_rows, weight, length, table_rows)

    return sent, keep


def on_device(tables, indices, weights, lengths):
    _, row_dev, feature_width = tables.shape
    batch_size = indices.shape[2]
    table_count = lax.axis_size("table")
    pair_count = lax.axis_size("pair")
    core = lax.axis_index("core").astype(jnp.int32)
    row = lax.axis_index("pair").astype(jnp.int32) * 2 + core
    index_rows = indices.transpose(1, 0, 2)
    sent, keep = kernels(tables[0], index_rows, weights[0], lengths, row * row_dev, core)
    received = lax.ppermute(sent, "core", [(0, 1), (1, 0)])
    partial = keep() + received
    share = batch_size // (table_count * pair_count * 2)
    tiles = partial.reshape(table_count * pair_count, share, feature_width)
    groups = [
        [(t * pair_count + (p ^ far_pair)) * 2 + c for t in range(table_count) for p in range(pair_count)]
        for c in range(2)
    ]
    arrived = lax.all_to_all(
        tiles,
        ("table", "pair", "core"),
        split_axis=0,
        concat_axis=0,
        axis_index_groups=groups,
        tiled=True,
    )
    shares = arrived.reshape(table_count, pair_count, share, feature_width)
    return shares.sum(axis=1).astype(jnp.bfloat16)


def solution(mesh):
    tables, rows = mesh.devices.shape
    by_core = Mesh(mesh.devices.reshape(tables, rows // 2, 2), ("table", "pair", "core"))
    row = ("pair", "core")
    placed = (
        P("table", row, None),
        P("table", None, None),
        P("table", None, None),
        P("table", None),
    )
    return jax.shard_map(
        on_device,
        mesh=by_core,
        in_specs=placed,
        out_specs=P(None, ("table", *row), None),
        check_vma=False,
    )
```

```python
import functools

import jax
import jax.numpy as jnp
from jax import lax
from jax.experimental import pallas as pl
from jax.experimental.pallas import tpu as pltpu
from jax.sharding import Mesh
from jax.sharding import PartitionSpec as P

lanes = 128
packed_rows = 16
slots = 16
weight_unit = 1024
far_pair = 26
vmem_bytes = 20 * 2**20


def read_positions(start_ref, index_ref, weight_ref, length_ref, rank_ref, code_ref, rows):
    bag, _, batch = index_ref.shape
    padded = rank_ref.shape[0]
    local = index_ref[:, 0, :] - start_ref[0]
    position = lax.broadcasted_iota(jnp.int32, (bag, batch), 0)
    inside = (local >= 0) & (local < rows) & (position < length_ref[...])
    code = local.astype(jnp.float32) * (2.0 * weight_unit)
    code = code + weight_ref[...].astype(jnp.float32) * weight_unit
    code_ref[:bag, :] = jnp.where(inside, code, 0.0)
    code_ref[bag:, :] = jnp.zeros((padded - bag, batch), jnp.float32)

    used = jnp.where(inside, 1.0, 0.0)
    used = jnp.concatenate([used, jnp.zeros((lanes - bag, batch), jnp.float32)], 0)
    before = lax.broadcasted_iota(jnp.int32, (padded, lanes), 0) > lax.broadcasted_iota(
        jnp.int32, (padded, lanes), 1
    )
    rank = jnp.dot(
        jnp.where(before, 1.0, 0.0).astype(jnp.bfloat16),
        used.astype(jnp.bfloat16),
        preferred_element_type=jnp.float32,
    )
    rank_ref[...] = rank
    return jnp.max(rank[padded - 1 :, :], keepdims=True)


def rounds_for(most):
    return (jnp.max(most).astype(jnp.int32) + (slots - 1)) // slots


def note_repeats(plane, repeated_ref):
    row = (plane.astype(jnp.int32) // (2 * weight_unit)).astype(jnp.float32)
    slot = lax.broadcasted_iota(jnp.int32, plane.shape, 0).astype(jnp.float32)
    row = jnp.where(plane > 0, row, -1.0 - slot)
    noted = []
    for first in range(0, plane.shape[0], slots):
        rows = row[first : first + slots]
        again = jnp.full(rows.shape, -1.0, jnp.float32)
        for shift in range(1, slots // 2 + 1):
            again = jnp.where(rows == pltpu.roll(rows, shift, 0), rows, again)
        noted.append((again.astype(jnp.int32) >> 8).astype(jnp.float32))
    for pair in range(repeated_ref.shape[0]):
        repeated_ref[pair : pair + 1, :] = any_in_pair(noted, pair)


def any_in_pair(noted, pair):
    hits = [jnp.where(pairs == float(pair), 1.0, 0.0) for pairs in noted]
    return jnp.max(functools.reduce(jnp.maximum, hits), axis=0, keepdims=True)


def note_later(plane, repeated_ref):
    pairs = (plane.astype(jnp.int32) // (2 * weight_unit)) >> 8
    noted = [jnp.where(plane > 0, pairs.astype(jnp.float32), -1.0)]
    for pair in range(repeated_ref.shape[0]):
        where = slice(pair, pair + 1)
        repeated_ref[where, :] = jnp.maximum(repeated_ref[where, :], any_in_pair(noted, pair))


def fill_slots(rank_ref, code_ref, slot_refs, first, note=None, repeated_ref=None):
    high_ref, low_ref, factor_ref = slot_refs
    groups = high_ref.shape[0]
    planes = []
    for block in range(rank_ref.shape[1] // lanes):
        where = pl.ds(block * lanes, lanes)
        rank = rank_ref[:, where]
        code = code_ref[:, where]
        for s in range(slots):
            at = rank == (first + s).astype(jnp.float32)
            planes.append(jnp.sum(jnp.where(at, code, 0.0), axis=0, keepdims=True))
    plane = jnp.concatenate(planes, 0)
    if note is not None:
        note(plane, repeated_ref)
    plane = jnp.concatenate([plane, pltpu.roll(plane, lanes - groups, 1)], 0)
    low_ref[...] = (plane.astype(jnp.int32) // (2 * weight_unit) % lanes).astype(jnp.float32)
    code = plane.T[:groups].astype(jnp.int32)
    row = code // (2 * weight_unit)
    high_ref[...] = (row // lanes).astype(jnp.float32)
    factor = (code % (2 * weight_unit)).astype(jnp.float32)
    factor_ref[...] = factor * (1.0 / weight_unit)


def spread_half(slot_refs, spread_ref, core, tiles, add):
    high_ref, low_ref, factor_ref = slot_refs
    group_bags = lanes // slots
    half_groups = high_ref.shape[0] // 2
    stride = spread_ref.shape[0] // tiles
    row_id = lax.broadcasted_iota(jnp.int32, (packed_rows, lanes), 0)
    row_ids = [
        (row_id + packed_rows * i).astype(jnp.float32).astype(jnp.bfloat16)
        for i in range(tiles // packed_rows)
    ]
    zero = jnp.zeros((packed_rows, lanes), jnp.bfloat16)
    lane = lax.broadcasted_iota(jnp.int32, (lanes, lanes), 1).astype(jnp.float32)
    lows = pltpu.roll(low_ref[...], (lanes - 2 * core) % lanes, 1)
    owner = lax.broadcasted_iota(jnp.int32, (packed_rows, lanes), 1) // slots
    owner = owner.astype(jnp.float32).astype(jnp.bfloat16)
    owned = [owner == jnp.full_like(owner, g) for g in range(group_bags)]

    def row_of(ref, j):
        row = ref[pl.ds(j, 1), :]
        return jnp.broadcast_to(row, (packed_rows, lanes)).astype(jnp.bfloat16)

    def spread_group(t):
        j = t // 2 * 4 + t % 2 + 2 * core
        high = row_of(high_ref, j)
        factor = row_of(factor_ref, j)
        at = [high == ids for ids in row_ids]
        by_high = []
        for g in range(group_bags):
            mine = jnp.where(owned[g], factor, zero)
            by_high += [jnp.where(hit, mine, zero) for hit in at]
        at_lane = t // 2 * 4 + t % 2
        low = jnp.broadcast_to(lows[:, at_lane : at_lane + 1], (lanes, lanes))
        by_low = jnp.where(low == lane, 1.0, 0.0).astype(jnp.bfloat16)
        total = lax.dot_general(
            jnp.concatenate(by_high, 0),
            by_low,
            (((1,), (0,)), ((), ())),
            preferred_element_type=jnp.float32,
        )
        blocks = group_bags // 2
        for g in range(group_bags):
            pair = (g // blocks * half_groups + t) // 2 ^ far_pair
            bag = g % blocks * 2 * half_groups + pair * 2 + t % 2
            where = pl.ds(bag, tiles, stride=stride)
            part = total[g * tiles : (g + 1) * tiles]
            if add:
                part = part + spread_ref[where, :]
            spread_ref[where, :] = part

    numbers = range(half_groups)
    if add:
        found = [jnp.max(factor_ref[pl.ds(t // 2 * 4 + t % 2 + 2 * core, 1), :]) for t in numbers]
        for t in numbers:
            pl.when(found[t] > 0)(functools.partial(spread_group, t))
    else:
        for t in numbers:
            spread_group(t)


def multiply(spread_ref, table_ref, repeated_ref, core, out_ref):
    tiles = table_ref.shape[0] // lanes
    stride = spread_ref.shape[0] // tiles
    bags = out_ref.shape[0]
    lane = lax.broadcasted_iota(jnp.int32, (1, lanes), 1)
    ours = (lane // 2) % 2 == core
    left = [
        jnp.where(ours, repeated_ref[pair : pair + 1, :], 0.0) for pair in range(tiles // 2)
    ]
    any_left = jnp.max(functools.reduce(jnp.maximum, left)) > 0
    left = [jnp.max(some) > 0 for some in left]
    factors = [
        spread_ref[pl.ds(i * stride, bags), :].astype(jnp.bfloat16) for i in range(tiles)
    ]
    out_ref[...] = jnp.dot(
        jnp.concatenate(factors, 1), table_ref[...], preferred_element_type=jnp.float32
    )

    def add_rest(pair):
        factors = [spread_ref[pl.ds((2 * pair + i) * stride, bags), :] for i in range(2)]
        factors = jnp.concatenate(factors, 1)
        rest = factors - factors.astype(jnp.bfloat16).astype(jnp.float32)
        out_ref[...] += jnp.dot(
            rest.astype(jnp.bfloat16),
            table_ref[pl.ds(2 * pair * lanes, 2 * lanes), :],
            preferred_element_type=jnp.float32,
        )

    @pl.when(any_left)
    def _():
        for pair in range(tiles // 2):
            pl.when(left[pair])(functools.partial(add_rest, pair))


def send_kernel(
    start_ref,
    core_ref,
    index_hbm,
    weight_hbm,
    length_hbm,
    table_hbm,
    out_ref,
    high_ref,
    low_ref,
    factor_ref,
    most_ref,
    repeated_ref,
    rank_ref,
    code_ref,
    table_ref,
    index_ref,
    weight_ref,
    length_ref,
    high_later,
    low_later,
    factor_later,
    spread_ref,
    table_sem,
    index_sem,
    weight_sem,
    length_sem,
):
    copies = [
        pltpu.make_async_copy(index_hbm, index_ref, index_sem),
        pltpu.make_async_copy(weight_hbm, weight_ref, weight_sem),
        pltpu.make_async_copy(length_hbm, length_ref, length_sem),
    ]
    for copy in copies:
        copy.start()
    for copy in copies:
        copy.wait()
    table_copy = pltpu.make_async_copy(table_hbm, table_ref, table_sem)
    table_copy.start()
    rows = table_ref.shape[0]
    tiles = rows // lanes
    core = 1 - core_ref[0]
    most = read_positions(
        start_ref, index_ref, weight_ref, length_ref, rank_ref, code_ref, rows
    )
    most_ref[...] = jnp.broadcast_to(most, most_ref.shape)
    rounds = rounds_for(most)
    slot_refs = (high_ref, low_ref, factor_ref)
    later_refs = (high_later, low_later, factor_later)
    fill_slots(rank_ref, code_ref, slot_refs, jnp.int32(0), note_repeats, repeated_ref)
    spread_half(slot_refs, spread_ref, core, tiles, False)

    def later_round(number, carry):
        fill_slots(rank_ref, code_ref, later_refs, number * slots, note_later, repeated_ref)
        spread_half(later_refs, spread_ref, core, tiles, True)
        return carry

    lax.fori_loop(1, rounds, later_round, 0)
    table_copy.wait()
    multiply(spread_ref, table_ref, repeated_ref, core, out_ref)


def keep_kernel(
    start_ref,
    core_ref,
    most_ref,
    repeated_ref,
    rank_ref,
    code_ref,
    high_ref,
    low_ref,
    factor_ref,
    table_hbm,
    out_ref,
    table_ref,
    high_later,
    low_later,
    factor_later,
    spread_ref,
    table_sem,
):
    table_copy = pltpu.make_async_copy(table_hbm, table_ref, table_sem)
    table_copy.start()
    rows = table_ref.shape[0]
    tiles = rows // lanes
    core = core_ref[0]
    slot_refs = (high_ref, low_ref, factor_ref)
    later_refs = (high_later, low_later, factor_later)
    spread_half(slot_refs, spread_ref, core, tiles, False)
    rounds = rounds_for(most_ref[...])

    def later_round(number, carry):
        fill_slots(rank_ref, code_ref, later_refs, number * slots)
        spread_half(later_refs, spread_ref, core, tiles, True)
        return carry

    lax.fori_loop(1, rounds, later_round, 0)
    table_copy.wait()
    multiply(spread_ref, table_ref, repeated_ref, core, out_ref)


def kernels(table_rows, index_rows, weight, length, row_start, core):
    rows, width = table_rows.shape
    bag, batch = weight.shape
    padded = bag + 8 - bag % 8
    groups = batch * slots // lanes
    half = batch // 2
    tiles = rows // lanes
    smem = pl.BlockSpec(memory_space=pltpu.SMEM)
    vmem = pl.BlockSpec(memory_space=pltpu.VMEM)
    far = pl.BlockSpec(memory_space=pl.ANY)
    table_scratch = pltpu.VMEM((rows, width), table_rows.dtype)
    by_position = jax.ShapeDtypeStruct((padded, batch), jnp.float32)
    by_group = [pltpu.VMEM((n, lanes), jnp.float32) for n in (groups, lanes, groups)]
    spread = pltpu.VMEM(((half + 1) * tiles, lanes), jnp.float32)
    dma = pltpu.SemaphoreType.DMA
    scratch = [
        table_scratch,
        pltpu.VMEM(index_rows.shape, index_rows.dtype),
        pltpu.VMEM(weight.shape, weight.dtype),
        pltpu.VMEM(length.shape, length.dtype),
        *by_group,
        spread,
        dma,
        dma,
        dma,
        dma,
    ]
    limit = pltpu.CompilerParams(vmem_limit_bytes=vmem_bytes)
    index_rows, weight, length, table_rows = [
        pltpu.with_memory_space_constraint(value, pltpu.HBM)
        for value in (index_rows, weight, length, table_rows)
    ]
    pools = jax.ShapeDtypeStruct((half, width), jnp.float32)
    slot = [jax.ShapeDtypeStruct((n, lanes), jnp.float32) for n in (groups, lanes, groups)]
    place = (row_start.reshape(1), core.reshape(1))

    sent, high, low, factor, most, repeated, rank, code = pl.pallas_call(
        send_kernel,
        out_shape=(
            pools,
            *slot,
            jax.ShapeDtypeStruct((8, lanes), jnp.float32),
            jax.ShapeDtypeStruct((tiles // 2, lanes), jnp.float32),
            by_position,
            by_position,
        ),
        in_specs=[smem, smem, far, far, far, far],
        out_specs=(vmem,) * 8,
        scratch_shapes=scratch,
        compiler_params=limit,
    )(*place, index_rows, weight, length, table_rows)

    def keep():
        return pl.pallas_call(
            keep_kernel,
            out_shape=pools,
            in_specs=[smem, smem, vmem, vmem, vmem, vmem, vmem, vmem, vmem, far],
            out_specs=vmem,
            scratch_shapes=[table_scratch, *by_group, spread, dma],
            compiler_params=limit,
            cost_estimate=pl.CostEstimate(
                flops=8 * half * rows * width, bytes_accessed=rows * width * 2, transcendentals=0
            ),
        )(*place, most, repeated, rank, code, high, low, factor, table_rows)

    return sent, keep


def on_device(tables, indices, weights, lengths):
    _, row_dev, feature_width = tables.shape
    batch_size = indices.shape[2]
    table_count = lax.axis_size("table")
    pair_count = lax.axis_size("pair")
    core = lax.axis_index("core").astype(jnp.int32)
    row = lax.axis_index("pair").astype(jnp.int32) * 2 + core
    index_rows = indices.transpose(1, 0, 2)
    sent, keep = kernels(tables[0], index_rows, weights[0], lengths, row * row_dev, core)
    received = lax.ppermute(sent, "core", [(0, 1), (1, 0)])
    partial = keep() + received
    share = batch_size // (table_count * pair_count * 2)
    tiles = partial.reshape(table_count * pair_count, share, feature_width)
    groups = [
        [(t * pair_count + (p ^ far_pair)) * 2 + c for t in range(table_count) for p in range(pair_count)]
        for c in range(2)
    ]
    arrived = lax.all_to_all(
        tiles,
        ("table", "pair", "core"),
        split_axis=0,
        concat_axis=0,
        axis_index_groups=groups,
        tiled=True,
    )
    shares = arrived.reshape(table_count, pair_count, share, feature_width)
    return shares.sum(axis=1).astype(jnp.bfloat16)


def solution(mesh):
    tables, rows = mesh.devices.shape
    by_core = Mesh(mesh.devices.reshape(tables, rows // 2, 2), ("table", "pair", "core"))
    row = ("pair", "core")
    placed = (
        P("table", row, None),
        P("table", None, None),
        P("table", None, None),
        P("table", None),
    )
    return jax.shard_map(
        on_device,
        mesh=by_core,
        in_specs=placed,
        out_specs=P(None, ("table", *row), None),
        check_vma=False,
    )
```

```python
import functools

import jax
import jax.numpy as jnp
from jax import lax
from jax.experimental import pallas as pl
from jax.experimental.pallas import tpu as pltpu
from jax.sharding import Mesh
from jax.sharding import PartitionSpec as P

lanes = 128
packed_rows = 16
slots = 16
weight_unit = 1024
far_pair = 26
vmem_bytes = 20 * 2**20


def read_positions(start_ref, index_ref, weight_ref, length_ref, rank_ref, code_ref, rows):
    bag, batch = weight_ref.shape
    padded = rank_ref.shape[0]
    blocks = [index_ref[block, :, 0, :] for block in range(batch // lanes)]
    local = jnp.concatenate(blocks, 1) - start_ref[0]
    position = lax.broadcasted_iota(jnp.int32, (bag, batch), 0)
    inside = (local >= 0) & (local < rows) & (position < length_ref[...])
    code = local.astype(jnp.float32) * (2.0 * weight_unit)
    code = code + weight_ref[...].astype(jnp.float32) * weight_unit
    code_ref[:bag, :] = jnp.where(inside, code, 0.0)
    code_ref[bag:, :] = jnp.zeros((padded - bag, batch), jnp.float32)

    used = jnp.where(inside, 1.0, 0.0)
    used = jnp.concatenate([used, jnp.zeros((lanes - bag, batch), jnp.float32)], 0)
    before = lax.broadcasted_iota(jnp.int32, (padded, lanes), 0) > lax.broadcasted_iota(
        jnp.int32, (padded, lanes), 1
    )
    rank = jnp.dot(
        jnp.where(before, 1.0, 0.0).astype(jnp.bfloat16),
        used.astype(jnp.bfloat16),
        preferred_element_type=jnp.float32,
    )
    rank_ref[...] = rank
    return jnp.max(rank[padded - 1 :, :], keepdims=True)


def rounds_for(most):
    return (jnp.max(most).astype(jnp.int32) + (slots - 1)) // slots


def note_repeats(plane, repeated_ref):
    row = (plane.astype(jnp.int32) // (2 * weight_unit)).astype(jnp.float32)
    slot = lax.broadcasted_iota(jnp.int32, plane.shape, 0).astype(jnp.float32)
    row = jnp.where(plane > 0, row, -1.0 - slot)
    noted = []
    for first in range(0, plane.shape[0], slots):
        rows = row[first : first + slots]
        again = jnp.full(rows.shape, -1.0, jnp.float32)
        for shift in range(1, slots // 2 + 1):
            again = jnp.where(rows == pltpu.roll(rows, shift, 0), rows, again)
        noted.append((again.astype(jnp.int32) >> 8).astype(jnp.float32))
    for pair in range(repeated_ref.shape[0]):
        repeated_ref[pair : pair + 1, :] = any_in_pair(noted, pair)


def any_in_pair(noted, pair):
    hits = [jnp.where(pairs == float(pair), 1.0, 0.0) for pairs in noted]
    return jnp.max(functools.reduce(jnp.maximum, hits), axis=0, keepdims=True)


def note_later(plane, repeated_ref):
    pairs = (plane.astype(jnp.int32) // (2 * weight_unit)) >> 8
    noted = [jnp.where(plane > 0, pairs.astype(jnp.float32), -1.0)]
    for pair in range(repeated_ref.shape[0]):
        where = slice(pair, pair + 1)
        repeated_ref[where, :] = jnp.maximum(repeated_ref[where, :], any_in_pair(noted, pair))


def fill_slots(rank_ref, code_ref, slot_refs, first):
    high_ref, low_ref, factor_ref = slot_refs
    groups = high_ref.shape[0]
    planes = []
    for block in range(rank_ref.shape[1] // lanes):
        where = pl.ds(block * lanes, lanes)
        rank = rank_ref[:, where]
        code = code_ref[:, where]
        for s in range(slots):
            at = rank == (first + s).astype(jnp.float32)
            planes.append(jnp.sum(jnp.where(at, code, 0.0), axis=0, keepdims=True))
    slot_codes = jnp.concatenate(planes, 0)
    plane = jnp.concatenate([slot_codes, pltpu.roll(slot_codes, lanes - groups, 1)], 0)
    low_ref[...] = (plane.astype(jnp.int32) // (2 * weight_unit) % lanes).astype(jnp.float32)
    code = plane.T[:groups].astype(jnp.int32)
    row = code // (2 * weight_unit)
    high_ref[...] = (row // lanes).astype(jnp.float32)
    factor = (code % (2 * weight_unit)).astype(jnp.float32)
    factor_ref[...] = factor * (1.0 / weight_unit)
    return slot_codes


def spread_half(slot_refs, spread_ref, core, tiles, add):
    high_ref, low_ref, factor_ref = slot_refs
    group_bags = lanes // slots
    half_groups = high_ref.shape[0] // 2
    stride = spread_ref.shape[0] // tiles
    row_id = lax.broadcasted_iota(jnp.int32, (packed_rows, lanes), 0)
    row_ids = [
        (row_id + packed_rows * i).astype(jnp.float32).astype(jnp.bfloat16)
        for i in range(tiles // packed_rows)
    ]
    zero = jnp.zeros((packed_rows, lanes), jnp.bfloat16)
    lane = lax.broadcasted_iota(jnp.int32, (lanes, lanes), 1).astype(jnp.float32)
    lows = pltpu.roll(low_ref[...], (lanes - 2 * core) % lanes, 1)
    owner = lax.broadcasted_iota(jnp.int32, (packed_rows, lanes), 1) // slots
    owner = owner.astype(jnp.float32).astype(jnp.bfloat16)
    owned = [owner == jnp.full_like(owner, g) for g in range(group_bags)]

    def row_of(ref, j):
        row = ref[pl.ds(j, 1), :]
        return jnp.broadcast_to(row, (packed_rows, lanes)).astype(jnp.bfloat16)

    def spread_group(t):
        j = t // 2 * 4 + t % 2 + 2 * core
        high = row_of(high_ref, j)
        factor = row_of(factor_ref, j)
        at = [high == ids for ids in row_ids]
        by_high = []
        for g in range(group_bags):
            mine = jnp.where(owned[g], factor, zero)
            by_high += [jnp.where(hit, mine, zero) for hit in at]
        at_lane = t // 2 * 4 + t % 2
        low = jnp.broadcast_to(lows[:, at_lane : at_lane + 1], (lanes, lanes))
        by_low = jnp.where(low == lane, 1.0, 0.0).astype(jnp.bfloat16)
        total = lax.dot_general(
            jnp.concatenate(by_high, 0),
            by_low,
            (((1,), (0,)), ((), ())),
            preferred_element_type=jnp.float32,
        )
        blocks = group_bags // 2
        for g in range(group_bags):
            pair = (g // blocks * half_groups + t) // 2 ^ far_pair
            bag = g % blocks * 2 * half_groups + pair * 2 + t % 2
            where = pl.ds(bag, tiles, stride=stride)
            part = total[g * tiles : (g + 1) * tiles]
            if add:
                part = part + spread_ref[where, :]
            spread_ref[where, :] = part

    numbers = range(half_groups)
    if add:
        found = [jnp.max(factor_ref[pl.ds(t // 2 * 4 + t % 2 + 2 * core, 1), :]) for t in numbers]
        for t in numbers:
            pl.when(found[t] > 0)(functools.partial(spread_group, t))
    else:
        for t in numbers:
            spread_group(t)


def multiply(spread_ref, table_ref, repeated_ref, core, out_ref):
    tiles = table_ref.shape[0] // lanes
    stride = spread_ref.shape[0] // tiles
    bags = out_ref.shape[0]
    lane = lax.broadcasted_iota(jnp.int32, (1, lanes), 1)
    ours = (lane // 2) % 2 == core
    left = [
        jnp.where(ours, repeated_ref[pair : pair + 1, :], 0.0) for pair in range(tiles // 2)
    ]
    any_left = jnp.max(functools.reduce(jnp.maximum, left)) > 0
    left = [jnp.max(some) > 0 for some in left]
    factors = [
        spread_ref[pl.ds(i * stride, bags), :].astype(jnp.bfloat16) for i in range(tiles)
    ]
    out_ref[...] = jnp.dot(
        jnp.concatenate(factors, 1), table_ref[...], preferred_element_type=jnp.float32
    )

    def add_rest(pair):
        factors = [spread_ref[pl.ds((2 * pair + i) * stride, bags), :] for i in range(2)]
        factors = jnp.concatenate(factors, 1)
        rest = factors - factors.astype(jnp.bfloat16).astype(jnp.float32)
        out_ref[...] += jnp.dot(
            rest.astype(jnp.bfloat16),
            table_ref[pl.ds(2 * pair * lanes, 2 * lanes), :],
            preferred_element_type=jnp.float32,
        )

    @pl.when(any_left)
    def _():
        for pair in range(tiles // 2):
            pl.when(left[pair])(functools.partial(add_rest, pair))


def send_kernel(
    start_ref,
    core_ref,
    index_hbm,
    weight_hbm,
    length_hbm,
    table_hbm,
    out_ref,
    high_ref,
    low_ref,
    factor_ref,
    most_ref,
    repeated_ref,
    rank_ref,
    code_ref,
    table_ref,
    index_ref,
    weight_ref,
    length_ref,
    high_later,
    low_later,
    factor_later,
    spread_ref,
    table_sem,
    index_sem,
    weight_sem,
    length_sem,
):
    copies = [
        *[
            pltpu.make_async_copy(
                index_hbm.at[:, :, pl.ds(block * lanes, lanes)],
                index_ref.at[block],
                index_sem.at[block],
            )
            for block in range(index_ref.shape[0])
        ],
        pltpu.make_async_copy(weight_hbm, weight_ref, weight_sem),
        pltpu.make_async_copy(length_hbm, length_ref, length_sem),
    ]
    for copy in copies:
        copy.start()
    for copy in copies:
        copy.wait()
    table_copy = pltpu.make_async_copy(table_hbm, table_ref, table_sem)
    table_copy.start()
    rows = table_ref.shape[0]
    tiles = rows // lanes
    core = 1 - core_ref[0]
    most = read_positions(
        start_ref, index_ref, weight_ref, length_ref, rank_ref, code_ref, rows
    )
    most_ref[...] = jnp.broadcast_to(most, most_ref.shape)
    rounds = rounds_for(most)
    slot_refs = (high_ref, low_ref, factor_ref)
    later_refs = (high_later, low_later, factor_later)
    plane = fill_slots(rank_ref, code_ref, slot_refs, jnp.int32(0))
    spread_half(slot_refs, spread_ref, core, tiles, False)
    note_repeats(plane, repeated_ref)

    def later_round(number, carry):
        note_later(fill_slots(rank_ref, code_ref, later_refs, number * slots), repeated_ref)
        spread_half(later_refs, spread_ref, core, tiles, True)
        return carry

    lax.fori_loop(1, rounds, later_round, 0)
    table_copy.wait()
    multiply(spread_ref, table_ref, repeated_ref, core, out_ref)


def keep_kernel(
    start_ref,
    core_ref,
    most_ref,
    repeated_ref,
    rank_ref,
    code_ref,
    high_ref,
    low_ref,
    factor_ref,
    table_ref,
    out_ref,
    high_later,
    low_later,
    factor_later,
    spread_ref,
):
    rows = table_ref.shape[0]
    tiles = rows // lanes
    core = core_ref[0]
    slot_refs = (high_ref, low_ref, factor_ref)
    later_refs = (high_later, low_later, factor_later)
    spread_half(slot_refs, spread_ref, core, tiles, False)
    rounds = rounds_for(most_ref[...])

    def later_round(number, carry):
        fill_slots(rank_ref, code_ref, later_refs, number * slots)
        spread_half(later_refs, spread_ref, core, tiles, True)
        return carry

    lax.fori_loop(1, rounds, later_round, 0)
    multiply(spread_ref, table_ref, repeated_ref, core, out_ref)


def kernels(table_rows, index_rows, weight, length, row_start, core):
    rows, width = table_rows.shape
    bag, batch = weight.shape
    padded = bag + 8 - bag % 8
    groups = batch * slots // lanes
    half = batch // 2
    tiles = rows // lanes
    smem = pl.BlockSpec(memory_space=pltpu.SMEM)
    vmem = pl.BlockSpec(memory_space=pltpu.VMEM)
    far = pl.BlockSpec(memory_space=pl.ANY)
    by_position = jax.ShapeDtypeStruct((padded, batch), jnp.float32)
    by_group = [pltpu.VMEM((n, lanes), jnp.float32) for n in (groups, lanes, groups)]
    spread = pltpu.VMEM(((half + 1) * tiles, lanes), jnp.float32)
    dma = pltpu.SemaphoreType.DMA
    scratch = [
        pltpu.VMEM((batch // lanes, bag, 1, lanes), index_rows.dtype),
        pltpu.VMEM(weight.shape, weight.dtype),
        pltpu.VMEM(length.shape, length.dtype),
        *by_group,
        spread,
        dma,
        dma((batch // lanes,)),
        dma,
        dma,
    ]
    limit = pltpu.CompilerParams(vmem_limit_bytes=vmem_bytes)
    index_rows, weight, length, table_rows = [
        pltpu.with_memory_space_constraint(value, pltpu.HBM)
        for value in (index_rows, weight, length, table_rows)
    ]
    pools = jax.ShapeDtypeStruct((half, width), jnp.float32)
    slot = [jax.ShapeDtypeStruct((n, lanes), jnp.float32) for n in (groups, lanes, groups)]
    place = (row_start.reshape(1), core.reshape(1))

    sent, high, low, factor, most, repeated, rank, code, table = pl.pallas_call(
        send_kernel,
        out_shape=(
            pools,
            *slot,
            jax.ShapeDtypeStruct((8, lanes), jnp.float32),
            jax.ShapeDtypeStruct((tiles // 2, lanes), jnp.float32),
            by_position,
            by_position,
            jax.ShapeDtypeStruct(table_rows.shape, table_rows.dtype),
        ),
        in_specs=[smem, smem, far, far, far, far],
        out_specs=(vmem,) * 9,
        scratch_shapes=scratch,
        compiler_params=limit,
    )(*place, index_rows, weight, length, table_rows)

    def keep():
        return pl.pallas_call(
            keep_kernel,
            out_shape=pools,
            in_specs=[smem, smem, *[vmem] * 8],
            out_specs=vmem,
            scratch_shapes=[*by_group, spread],
            compiler_params=limit,
            cost_estimate=pl.CostEstimate(
                flops=8 * half * rows * width, bytes_accessed=rows * width * 2, transcendentals=0
            ),
        )(*place, most, repeated, rank, code, high, low, factor, table)

    return sent, keep


def on_device(tables, indices, weights, lengths):
    _, row_dev, feature_width = tables.shape
    batch_size = indices.shape[2]
    table_count = lax.axis_size("table")
    pair_count = lax.axis_size("pair")
    core = lax.axis_index("core").astype(jnp.int32)
    row = lax.axis_index("pair").astype(jnp.int32) * 2 + core
    index_rows = indices.transpose(1, 0, 2)
    sent, keep = kernels(tables[0], index_rows, weights[0], lengths, row * row_dev, core)
    received = lax.ppermute(sent, "core", [(0, 1), (1, 0)])
    partial = keep() + received
    share = batch_size // (table_count * pair_count * 2)
    tiles = partial.reshape(table_count * pair_count, share, feature_width)
    groups = [
        [(t * pair_count + (p ^ far_pair)) * 2 + c for t in range(table_count) for p in range(pair_count)]
        for c in range(2)
    ]
    arrived = lax.all_to_all(
        tiles,
        ("table", "pair", "core"),
        split_axis=0,
        concat_axis=0,
        axis_index_groups=groups,
        tiled=True,
    )
    shares = arrived.reshape(table_count, pair_count, share, feature_width)
    return shares.sum(axis=1).astype(jnp.bfloat16)


def solution(mesh):
    tables, rows = mesh.devices.shape
    by_core = Mesh(mesh.devices.reshape(tables, rows // 2, 2), ("table", "pair", "core"))
    row = ("pair", "core")
    placed = (
        P("table", row, None),
        P("table", None, None),
        P("table", None, None),
        P("table", None),
    )
    return jax.shard_map(
        on_device,
        mesh=by_core,
        in_specs=placed,
        out_specs=P(None, ("table", *row), None),
        check_vma=False,
    )
```

```python
import functools

import jax
import jax.numpy as jnp
from jax import lax
from jax.experimental import pallas as pl
from jax.experimental.pallas import tpu as pltpu
from jax.sharding import Mesh
from jax.sharding import PartitionSpec as P

lanes = 128
packed_rows = 16
slots = 16
weight_unit = 1024
far_pair = 26
vmem_bytes = 20 * 2**20


def read_positions(start_ref, index_ref, weight_ref, length_ref, rank_ref, code_ref, rows):
    bag, _, batch = index_ref.shape
    padded = rank_ref.shape[0]
    local = index_ref[:, 0, :] - start_ref[0]
    position = lax.broadcasted_iota(jnp.int32, (bag, batch), 0)
    inside = (local >= 0) & (local < rows) & (position < length_ref[...])
    code = local.astype(jnp.float32) * (2.0 * weight_unit)
    code = code + weight_ref[...].astype(jnp.float32) * weight_unit
    code_ref[:bag, :] = jnp.where(inside, code, 0.0)
    code_ref[bag:, :] = jnp.zeros((padded - bag, batch), jnp.float32)

    used = jnp.where(inside, 1.0, 0.0)
    used = jnp.concatenate([used, jnp.zeros((lanes - bag, batch), jnp.float32)], 0)
    before = lax.broadcasted_iota(jnp.int32, (padded, lanes), 0) > lax.broadcasted_iota(
        jnp.int32, (padded, lanes), 1
    )
    rank = jnp.dot(
        jnp.where(before, 1.0, 0.0).astype(jnp.bfloat16),
        used.astype(jnp.bfloat16),
        preferred_element_type=jnp.float32,
    )
    rank_ref[...] = rank
    return jnp.max(rank[padded - 1 :, :], keepdims=True)


def rounds_for(most):
    return (jnp.max(most).astype(jnp.int32) + (slots - 1)) // slots


def note_repeats(plane, repeated_ref):
    row = (plane.astype(jnp.int32) // (2 * weight_unit)).astype(jnp.float32)
    slot = lax.broadcasted_iota(jnp.int32, plane.shape, 0).astype(jnp.float32)
    row = jnp.where(plane > 0, row, -1.0 - slot)
    noted = []
    for first in range(0, plane.shape[0], slots):
        rows = row[first : first + slots]
        again = jnp.full(rows.shape, -1.0, jnp.float32)
        for shift in range(1, slots // 2 + 1):
            again = jnp.where(rows == pltpu.roll(rows, shift, 0), rows, again)
        noted.append((again.astype(jnp.int32) >> 8).astype(jnp.float32))
    for pair in range(repeated_ref.shape[0]):
        repeated_ref[pair : pair + 1, :] = any_in_pair(noted, pair)


def any_in_pair(noted, pair):
    hits = [jnp.where(pairs == float(pair), 1.0, 0.0) for pairs in noted]
    return jnp.max(functools.reduce(jnp.maximum, hits), axis=0, keepdims=True)


def note_later(plane, repeated_ref):
    pairs = (plane.astype(jnp.int32) // (2 * weight_unit)) >> 8
    noted = [jnp.where(plane > 0, pairs.astype(jnp.float32), -1.0)]
    for pair in range(repeated_ref.shape[0]):
        where = slice(pair, pair + 1)
        repeated_ref[where, :] = jnp.maximum(repeated_ref[where, :], any_in_pair(noted, pair))


def fill_slots(rank_ref, code_ref, slot_refs, first, note=None, repeated_ref=None):
    planes = []
    for block, (high_ref, low_ref, factor_ref) in enumerate(slot_refs):
        rows = high_ref.shape[0]
        where = pl.ds(block * lanes, lanes)
        rank = rank_ref[:, where]
        code = code_ref[:, where]
        filled = []
        for s in range(slots):
            at = rank == (first + s).astype(jnp.float32)
            filled.append(jnp.sum(jnp.where(at, code, 0.0), axis=0, keepdims=True))
        plane = jnp.concatenate(filled, 0)
        planes.append(plane)
        shifts = [(lanes - rows * g) % lanes for g in range(lanes // rows)]
        plane = jnp.concatenate([pltpu.roll(plane, n, 1) if n else plane for n in shifts], 0)
        low_ref[...] = (plane.astype(jnp.int32) // (2 * weight_unit) % lanes).astype(jnp.float32)
        code = plane.T[:rows].astype(jnp.int32)
        row = code // (2 * weight_unit)
        high_ref[...] = (row // lanes).astype(jnp.float32)
        factor = (code % (2 * weight_unit)).astype(jnp.float32)
        factor_ref[...] = factor * (1.0 / weight_unit)
    if note is not None:
        note(jnp.concatenate(planes, 0), repeated_ref)


def spread_half(slot_refs, spread_ref, core, tiles, add):
    group_bags = lanes // slots
    block_groups = slots // 2
    stride = spread_ref.shape[0] // tiles
    row_id = lax.broadcasted_iota(jnp.int32, (packed_rows, lanes), 0)
    row_ids = [
        (row_id + packed_rows * i).astype(jnp.float32).astype(jnp.bfloat16)
        for i in range(tiles // packed_rows)
    ]
    zero = jnp.zeros((packed_rows, lanes), jnp.bfloat16)
    lane = lax.broadcasted_iota(jnp.int32, (lanes, lanes), 1).astype(jnp.float32)
    lows = [
        pltpu.roll(low_ref[...], (lanes - 2 * core) % lanes, 1) for _, low_ref, _ in slot_refs
    ]
    owner = lax.broadcasted_iota(jnp.int32, (packed_rows, lanes), 1) // slots
    owner = owner.astype(jnp.float32).astype(jnp.bfloat16)
    owned = [owner == jnp.full_like(owner, g) for g in range(group_bags)]

    def row_of(ref, j):
        row = ref[pl.ds(j, 1), :]
        return jnp.broadcast_to(row, (packed_rows, lanes)).astype(jnp.bfloat16)

    def spread_group(block, t):
        high_ref, _, factor_ref = slot_refs[block]
        j = t // 2 * 4 + t % 2 + 2 * core
        high = row_of(high_ref, j)
        factor = row_of(factor_ref, j)
        at = [high == ids for ids in row_ids]
        by_high = []
        for g in range(group_bags):
            mine = jnp.where(owned[g], factor, zero)
            by_high += [jnp.where(hit, mine, zero) for hit in at]
        at_lane = t // 2 * 4 + t % 2
        low = jnp.broadcast_to(lows[block][:, at_lane : at_lane + 1], (lanes, lanes))
        by_low = jnp.where(low == lane, 1.0, 0.0).astype(jnp.bfloat16)
        total = lax.dot_general(
            jnp.concatenate(by_high, 0),
            by_low,
            (((1,), (0,)), ((), ())),
            preferred_element_type=jnp.float32,
        )
        for g in range(group_bags):
            pair = (g * block_groups + t) // 2 ^ far_pair
            bag = block * lanes // 2 + pair * 2 + t % 2
            where = pl.ds(bag, tiles, stride=stride)
            part = total[g * tiles : (g + 1) * tiles]
            if add:
                part = part + spread_ref[where, :]
            spread_ref[where, :] = part

    numbers = [(block, t) for block in range(len(slot_refs)) for t in range(block_groups)]
    if add:
        found = []
        for block, t in numbers:
            factors = slot_refs[block][2][pl.ds(t // 2 * 4 + t % 2 + 2 * core, 1), :]
            found.append(jnp.max(factors))
        for number, some in zip(numbers, found):
            pl.when(some > 0)(functools.partial(spread_group, *number))
    else:
        for number in numbers:
            spread_group(*number)


def multiply(spread_ref, table_ref, repeated_ref, core, out_ref):
    tiles = table_ref.shape[0] // lanes
    stride = spread_ref.shape[0] // tiles
    bags = out_ref.shape[0]
    lane = lax.broadcasted_iota(jnp.int32, (1, lanes), 1)
    ours = (lane // 2) % 2 == core
    left = [
        jnp.where(ours, repeated_ref[pair : pair + 1, :], 0.0) for pair in range(tiles // 2)
    ]
    any_left = jnp.max(functools.reduce(jnp.maximum, left)) > 0
    left = [jnp.max(some) > 0 for some in left]
    factors = [
        spread_ref[pl.ds(i * stride, bags), :].astype(jnp.bfloat16) for i in range(tiles)
    ]
    out_ref[...] = jnp.dot(
        jnp.concatenate(factors, 1), table_ref[...], preferred_element_type=jnp.float32
    )

    def add_rest(pair):
        factors = [spread_ref[pl.ds((2 * pair + i) * stride, bags), :] for i in range(2)]
        factors = jnp.concatenate(factors, 1)
        rest = factors - factors.astype(jnp.bfloat16).astype(jnp.float32)
        out_ref[...] += jnp.dot(
            rest.astype(jnp.bfloat16),
            table_ref[pl.ds(2 * pair * lanes, 2 * lanes), :],
            preferred_element_type=jnp.float32,
        )

    @pl.when(any_left)
    def _():
        for pair in range(tiles // 2):
            pl.when(left[pair])(functools.partial(add_rest, pair))


def by_block(refs):
    return [refs[i : i + 3] for i in range(0, len(refs), 3)]


def send_kernel(blocks, *refs):
    start_ref, core_ref, index_hbm, weight_hbm, length_hbm, table_hbm, *refs = refs
    out_ref, most_ref, repeated_ref, rank_ref, code_ref, *refs = refs
    slot_refs = by_block(refs[: 3 * blocks])
    later_refs = by_block(refs[3 * blocks : 6 * blocks])
    index_ref, weight_ref, length_ref, table_ref, spread_ref, *sems = refs[6 * blocks :]
    table_sem, index_sem, weight_sem, length_sem = sems
    copies = [
        pltpu.make_async_copy(index_hbm, index_ref, index_sem),
        pltpu.make_async_copy(weight_hbm, weight_ref, weight_sem),
        pltpu.make_async_copy(length_hbm, length_ref, length_sem),
    ]
    for copy in copies:
        copy.start()
    for copy in copies:
        copy.wait()
    table_copy = pltpu.make_async_copy(table_hbm, table_ref, table_sem)
    table_copy.start()
    rows = table_ref.shape[0]
    tiles = rows // lanes
    core = 1 - core_ref[0]
    most = read_positions(
        start_ref, index_ref, weight_ref, length_ref, rank_ref, code_ref, rows
    )
    most_ref[...] = jnp.broadcast_to(most, most_ref.shape)
    rounds = rounds_for(most)
    fill_slots(rank_ref, code_ref, slot_refs, jnp.int32(0), note_repeats, repeated_ref)
    spread_half(slot_refs, spread_ref, core, tiles, False)

    def later_round(number, carry):
        fill_slots(rank_ref, code_ref, later_refs, number * slots, note_later, repeated_ref)
        spread_half(later_refs, spread_ref, core, tiles, True)
        return carry

    lax.fori_loop(1, rounds, later_round, 0)
    table_copy.wait()
    multiply(spread_ref, table_ref, repeated_ref, core, out_ref)


def keep_kernel(blocks, *refs):
    start_ref, core_ref, most_ref, repeated_ref, rank_ref, code_ref, *refs = refs
    slot_refs = by_block(refs[: 3 * blocks])
    table_hbm, out_ref, *refs = refs[3 * blocks :]
    later_refs = by_block(refs[: 3 * blocks])
    table_ref, spread_ref, table_sem = refs[3 * blocks :]
    table_copy = pltpu.make_async_copy(table_hbm, table_ref, table_sem)
    table_copy.start()
    tiles = table_ref.shape[0] // lanes
    core = core_ref[0]
    spread_half(slot_refs, spread_ref, core, tiles, False)
    rounds = rounds_for(most_ref[...])

    def later_round(number, carry):
        fill_slots(rank_ref, code_ref, later_refs, number * slots)
        spread_half(later_refs, spread_ref, core, tiles, True)
        return carry

    lax.fori_loop(1, rounds, later_round, 0)
    table_copy.wait()
    multiply(spread_ref, table_ref, repeated_ref, core, out_ref)


def kernels(table_rows, index_rows, weight, length, row_start, core):
    rows, width = table_rows.shape
    bag, batch = weight.shape
    padded = bag + 8 - bag % 8
    half = batch // 2
    tiles = rows // lanes
    blocks = batch // lanes
    smem = pl.BlockSpec(memory_space=pltpu.SMEM)
    vmem = pl.BlockSpec(memory_space=pltpu.VMEM)
    far = pl.BlockSpec(memory_space=pl.ANY)
    by_position = jax.ShapeDtypeStruct((padded, batch), jnp.float32)
    slot_shapes = [(n, lanes) for n in (slots, lanes, slots)] * blocks
    slot = [jax.ShapeDtypeStruct(shape, jnp.float32) for shape in slot_shapes]
    later = [pltpu.VMEM(shape, jnp.float32) for shape in slot_shapes]
    table_scratch = pltpu.VMEM((rows, width), table_rows.dtype)
    spread = pltpu.VMEM(((half + 1) * tiles, lanes), jnp.float32)
    dma = pltpu.SemaphoreType.DMA
    limit = pltpu.CompilerParams(vmem_limit_bytes=vmem_bytes)
    index_rows, weight, length, table_rows = [
        pltpu.with_memory_space_constraint(value, pltpu.HBM)
        for value in (index_rows, weight, length, table_rows)
    ]
    pools = jax.ShapeDtypeStruct((half, width), jnp.float32)
    place = (row_start.reshape(1), core.reshape(1))

    sent, most, repeated, rank, code, *slot_values = pl.pallas_call(
        functools.partial(send_kernel, blocks),
        out_shape=(
            pools,
            jax.ShapeDtypeStruct((8, lanes), jnp.float32),
            jax.ShapeDtypeStruct((tiles // 2, lanes), jnp.float32),
            by_position,
            by_position,
            *slot,
        ),
        in_specs=[smem, smem, far, far, far, far],
        out_specs=(vmem,) * (5 + len(slot)),
        scratch_shapes=[
            *later,
            pltpu.VMEM(index_rows.shape, index_rows.dtype),
            pltpu.VMEM(weight.shape, weight.dtype),
            pltpu.VMEM(length.shape, length.dtype),
            table_scratch,
            spread,
            dma,
            dma,
            dma,
            dma,
        ],
        compiler_params=limit,
    )(*place, index_rows, weight, length, table_rows)

    def keep():
        return pl.pallas_call(
            functools.partial(keep_kernel, blocks),
            out_shape=pools,
            in_specs=[smem, smem, *[vmem] * (4 + len(slot)), far],
            out_specs=vmem,
            scratch_shapes=[*later, table_scratch, spread, dma],
            compiler_params=limit,
            cost_estimate=pl.CostEstimate(
                flops=8 * half * rows * width, bytes_accessed=rows * width * 2, transcendentals=0
            ),
        )(*place, most, repeated, rank, code, *slot_values, table_rows)

    return sent, keep


def on_device(tables, indices, weights, lengths):
    _, row_dev, feature_width = tables.shape
    batch_size = indices.shape[2]
    table_count = lax.axis_size("table")
    pair_count = lax.axis_size("pair")
    core = lax.axis_index("core").astype(jnp.int32)
    row = lax.axis_index("pair").astype(jnp.int32) * 2 + core
    index_rows = indices.transpose(1, 0, 2)
    sent, keep = kernels(tables[0], index_rows, weights[0], lengths, row * row_dev, core)
    received = lax.ppermute(sent, "core", [(0, 1), (1, 0)])
    partial = keep() + received
    share = batch_size // (table_count * pair_count * 2)
    tiles = partial.reshape(table_count * pair_count, share, feature_width)
    groups = [
        [(t * pair_count + (p ^ far_pair)) * 2 + c for t in range(table_count) for p in range(pair_count)]
        for c in range(2)
    ]
    arrived = lax.all_to_all(
        tiles,
        ("table", "pair", "core"),
        split_axis=0,
        concat_axis=0,
        axis_index_groups=groups,
        tiled=True,
    )
    shares = arrived.reshape(table_count, pair_count, share, feature_width)
    return shares.sum(axis=1).astype(jnp.bfloat16)


def solution(mesh):
    tables, rows = mesh.devices.shape
    by_core = Mesh(mesh.devices.reshape(tables, rows // 2, 2), ("table", "pair", "core"))
    row = ("pair", "core")
    placed = (
        P("table", row, None),
        P("table", None, None),
        P("table", None, None),
        P("table", None),
    )
    return jax.shard_map(
        on_device,
        mesh=by_core,
        in_specs=placed,
        out_specs=P(None, ("table", *row), None),
        check_vma=False,
    )
```

```python
import functools

import jax
import jax.numpy as jnp
from jax import lax
from jax.experimental import pallas as pl
from jax.experimental.pallas import tpu as pltpu
from jax.sharding import Mesh
from jax.sharding import PartitionSpec as P

lanes = 128
packed_rows = 16
slots = 16
weight_unit = 1024
far_pair = 26
vmem_bytes = 20 * 2**20


def read_positions(start_ref, index_ref, weight_ref, length_ref, rank_ref, code_ref, rows):
    bag, _, batch = index_ref.shape
    padded = rank_ref.shape[0]
    local = index_ref[:, 0, :] - start_ref[0]
    position = lax.broadcasted_iota(jnp.int32, (bag, batch), 0)
    inside = (local >= 0) & (local < rows) & (position < length_ref[...])
    code = local.astype(jnp.float32) * (2.0 * weight_unit)
    code = code + weight_ref[...].astype(jnp.float32) * weight_unit
    code_ref[:bag, :] = jnp.where(inside, code, 0.0)
    code_ref[bag:, :] = jnp.zeros((padded - bag, batch), jnp.float32)

    used = jnp.where(inside, 1.0, 0.0)
    used = jnp.concatenate([used, jnp.zeros((lanes - bag, batch), jnp.float32)], 0)
    before = lax.broadcasted_iota(jnp.int32, (padded, lanes), 0) > lax.broadcasted_iota(
        jnp.int32, (padded, lanes), 1
    )
    rank = jnp.dot(
        jnp.where(before, 1.0, 0.0).astype(jnp.bfloat16),
        used.astype(jnp.bfloat16),
        preferred_element_type=jnp.float32,
    )
    rank_ref[...] = rank
    return jnp.max(rank[padded - 1 :, :], keepdims=True)


def rounds_for(most):
    return (jnp.max(most).astype(jnp.int32) + (slots - 1)) // slots


def note_repeats(plane, repeated_ref):
    row = (plane.astype(jnp.int32) // (2 * weight_unit)).astype(jnp.float32)
    slot = lax.broadcasted_iota(jnp.int32, plane.shape, 0).astype(jnp.float32)
    row = jnp.where(plane > 0, row, -1.0 - slot)
    noted = []
    for first in range(0, plane.shape[0], slots):
        rows = row[first : first + slots]
        again = jnp.full(rows.shape, -1.0, jnp.float32)
        for shift in range(1, slots // 2 + 1):
            again = jnp.where(rows == pltpu.roll(rows, shift, 0), rows, again)
        noted.append((again.astype(jnp.int32) >> 8).astype(jnp.float32))
    for pair in range(repeated_ref.shape[0]):
        repeated_ref[pair : pair + 1, :] = any_in_pair(noted, pair)


def any_in_pair(noted, pair):
    hits = [jnp.where(pairs == float(pair), 1.0, 0.0) for pairs in noted]
    return jnp.max(functools.reduce(jnp.maximum, hits), axis=0, keepdims=True)


def note_later(plane, repeated_ref):
    pairs = (plane.astype(jnp.int32) // (2 * weight_unit)) >> 8
    noted = [jnp.where(plane > 0, pairs.astype(jnp.float32), -1.0)]
    for pair in range(repeated_ref.shape[0]):
        where = slice(pair, pair + 1)
        repeated_ref[where, :] = jnp.maximum(repeated_ref[where, :], any_in_pair(noted, pair))


def fill_slots(rank_ref, code_ref, slot_refs, first):
    high_ref, low_ref, factor_ref = slot_refs
    groups = high_ref.shape[0]
    planes = []
    for block in range(rank_ref.shape[1] // lanes):
        where = pl.ds(block * lanes, lanes)
        rank = rank_ref[:, where]
        code = code_ref[:, where]
        for s in range(slots):
            at = rank == (first + s).astype(jnp.float32)
            planes.append(jnp.sum(jnp.where(at, code, 0.0), axis=0, keepdims=True))
    slot_codes = jnp.concatenate(planes, 0)
    plane = jnp.concatenate([slot_codes, pltpu.roll(slot_codes, lanes - groups, 1)], 0)
    low_ref[...] = (plane.astype(jnp.int32) // (2 * weight_unit) % lanes).astype(jnp.float32)
    code = plane.T[:groups].astype(jnp.int32)
    row = code // (2 * weight_unit)
    high_ref[...] = (row // lanes).astype(jnp.float32)
    factor = (code % (2 * weight_unit)).astype(jnp.float32)
    factor_ref[...] = factor * (1.0 / weight_unit)
    return slot_codes


def spread_half(slot_refs, spread_ref, core, tiles, add):
    high_ref, low_ref, factor_ref = slot_refs
    group_bags = lanes // slots
    half_groups = high_ref.shape[0] // 2
    stride = spread_ref.shape[0] // tiles
    row_id = lax.broadcasted_iota(jnp.int32, (packed_rows, lanes), 0)
    row_ids = [
        (row_id + packed_rows * i).astype(jnp.float32).astype(jnp.bfloat16)
        for i in range(tiles // packed_rows)
    ]
    zero = jnp.zeros((packed_rows, lanes), jnp.bfloat16)
    lane = lax.broadcasted_iota(jnp.int32, (lanes, lanes), 1).astype(jnp.float32)
    lows = pltpu.roll(low_ref[...], (lanes - 2 * core) % lanes, 1)
    owner = lax.broadcasted_iota(jnp.int32, (packed_rows, lanes), 1) // slots
    owner = owner.astype(jnp.float32).astype(jnp.bfloat16)
    owned = [owner == jnp.full_like(owner, g) for g in range(group_bags)]

    def row_of(ref, j):
        row = ref[pl.ds(j, 1), :]
        return jnp.broadcast_to(row, (packed_rows, lanes)).astype(jnp.bfloat16)

    def spread_group(t):
        j = t // 2 * 4 + t % 2 + 2 * core
        high = row_of(high_ref, j)
        factor = row_of(factor_ref, j)
        at = [high == ids for ids in row_ids]
        by_high = []
        for g in range(group_bags):
            mine = jnp.where(owned[g], factor, zero)
            by_high += [jnp.where(hit, mine, zero) for hit in at]
        at_lane = t // 2 * 4 + t % 2
        low = jnp.broadcast_to(lows[:, at_lane : at_lane + 1], (lanes, lanes))
        by_low = jnp.where(low == lane, 1.0, 0.0).astype(jnp.bfloat16)
        total = lax.dot_general(
            jnp.concatenate(by_high, 0),
            by_low,
            (((1,), (0,)), ((), ())),
            preferred_element_type=jnp.float32,
        )
        blocks = group_bags // 2
        for g in range(group_bags):
            pair = (g // blocks * half_groups + t) // 2 ^ far_pair
            bag = g % blocks * 2 * half_groups + pair * 2 + t % 2
            where = pl.ds(bag, tiles, stride=stride)
            part = total[g * tiles : (g + 1) * tiles]
            if add:
                part = part + spread_ref[where, :]
            spread_ref[where, :] = part

    numbers = range(half_groups)
    if add:
        found = [jnp.max(factor_ref[pl.ds(t // 2 * 4 + t % 2 + 2 * core, 1), :]) for t in numbers]
        for t in numbers:
            pl.when(found[t] > 0)(functools.partial(spread_group, t))
    else:
        for t in numbers:
            spread_group(t)


def multiply(spread_ref, table_ref, repeated_ref, core, out_ref):
    tiles = table_ref.shape[0] // lanes
    stride = spread_ref.shape[0] // tiles
    bags = out_ref.shape[0]
    lane = lax.broadcasted_iota(jnp.int32, (1, lanes), 1)
    ours = (lane // 2) % 2 == core
    left = [
        jnp.where(ours, repeated_ref[pair : pair + 1, :], 0.0) for pair in range(tiles // 2)
    ]
    left_in_four = [
        jnp.max(functools.reduce(jnp.maximum, left[i : i + 4])) > 0 for i in range(0, len(left), 4)
    ]
    left = [jnp.max(some) > 0 for some in left]
    factors = [
        spread_ref[pl.ds(i * stride, bags), :].astype(jnp.bfloat16) for i in range(tiles)
    ]
    out_ref[...] = jnp.dot(
        jnp.concatenate(factors, 1), table_ref[...], preferred_element_type=jnp.float32
    )

    def add_rest(pair):
        factors = [spread_ref[pl.ds((2 * pair + i) * stride, bags), :] for i in range(2)]
        factors = jnp.concatenate(factors, 1)
        rest = factors - factors.astype(jnp.bfloat16).astype(jnp.float32)
        out_ref[...] += jnp.dot(
            rest.astype(jnp.bfloat16),
            table_ref[pl.ds(2 * pair * lanes, 2 * lanes), :],
            preferred_element_type=jnp.float32,
        )

    for four in range(tiles // 8):

        @pl.when(left_in_four[four])
        def _(four=four):
            for pair in range(4 * four, 4 * four + 4):
                pl.when(left[pair])(functools.partial(add_rest, pair))


def send_kernel(
    start_ref,
    core_ref,
    index_hbm,
    weight_hbm,
    length_hbm,
    table_hbm,
    out_ref,
    high_ref,
    low_ref,
    factor_ref,
    most_ref,
    repeated_ref,
    rank_ref,
    code_ref,
    table_ref,
    index_ref,
    weight_ref,
    length_ref,
    high_later,
    low_later,
    factor_later,
    spread_ref,
    table_sem,
    index_sem,
    weight_sem,
    length_sem,
):
    copies = [
        pltpu.make_async_copy(index_hbm, index_ref, index_sem),
        pltpu.make_async_copy(weight_hbm, weight_ref, weight_sem),
        pltpu.make_async_copy(length_hbm, length_ref, length_sem),
    ]
    for copy in copies:
        copy.start()
    for copy in copies:
        copy.wait()
    table_copy = pltpu.make_async_copy(table_hbm, table_ref, table_sem)
    table_copy.start()
    rows = table_ref.shape[0]
    tiles = rows // lanes
    core = 1 - core_ref[0]
    most = read_positions(
        start_ref, index_ref, weight_ref, length_ref, rank_ref, code_ref, rows
    )
    most_ref[...] = jnp.broadcast_to(most, most_ref.shape)
    rounds = rounds_for(most)
    slot_refs = (high_ref, low_ref, factor_ref)
    later_refs = (high_later, low_later, factor_later)
    plane = fill_slots(rank_ref, code_ref, slot_refs, jnp.int32(0))
    spread_half(slot_refs, spread_ref, core, tiles, False)
    note_repeats(plane, repeated_ref)

    def later_round(number, carry):
        note_later(fill_slots(rank_ref, code_ref, later_refs, number * slots), repeated_ref)
        spread_half(later_refs, spread_ref, core, tiles, True)
        return carry

    lax.fori_loop(1, rounds, later_round, 0)
    table_copy.wait()
    multiply(spread_ref, table_ref, repeated_ref, core, out_ref)


def keep_kernel(
    start_ref,
    core_ref,
    most_ref,
    repeated_ref,
    rank_ref,
    code_ref,
    high_ref,
    low_ref,
    factor_ref,
    table_hbm,
    out_ref,
    table_ref,
    high_later,
    low_later,
    factor_later,
    spread_ref,
    table_sem,
):
    table_copy = pltpu.make_async_copy(table_hbm, table_ref, table_sem)
    table_copy.start()
    rows = table_ref.shape[0]
    tiles = rows // lanes
    core = core_ref[0]
    slot_refs = (high_ref, low_ref, factor_ref)
    later_refs = (high_later, low_later, factor_later)
    spread_half(slot_refs, spread_ref, core, tiles, False)
    rounds = rounds_for(most_ref[...])

    def later_round(number, carry):
        fill_slots(rank_ref, code_ref, later_refs, number * slots)
        spread_half(later_refs, spread_ref, core, tiles, True)
        return carry

    lax.fori_loop(1, rounds, later_round, 0)
    table_copy.wait()
    multiply(spread_ref, table_ref, repeated_ref, core, out_ref)


def kernels(table_rows, index_rows, weight, length, row_start, core):
    rows, width = table_rows.shape
    bag, batch = weight.shape
    padded = bag + 8 - bag % 8
    groups = batch * slots // lanes
    half = batch // 2
    tiles = rows // lanes
    smem = pl.BlockSpec(memory_space=pltpu.SMEM)
    vmem = pl.BlockSpec(memory_space=pltpu.VMEM)
    far = pl.BlockSpec(memory_space=pl.ANY)
    table_scratch = pltpu.VMEM((rows, width), table_rows.dtype)
    by_position = jax.ShapeDtypeStruct((padded, batch), jnp.float32)
    by_group = [pltpu.VMEM((n, lanes), jnp.float32) for n in (groups, lanes, groups)]
    spread = pltpu.VMEM(((half + 1) * tiles, lanes), jnp.float32)
    dma = pltpu.SemaphoreType.DMA
    scratch = [
        table_scratch,
        pltpu.VMEM(index_rows.shape, index_rows.dtype),
        pltpu.VMEM(weight.shape, weight.dtype),
        pltpu.VMEM(length.shape, length.dtype),
        *by_group,
        spread,
        dma,
        dma,
        dma,
        dma,
    ]
    limit = pltpu.CompilerParams(vmem_limit_bytes=vmem_bytes)
    index_rows, weight, length, table_rows = [
        pltpu.with_memory_space_constraint(value, pltpu.HBM)
        for value in (index_rows, weight, length, table_rows)
    ]
    pools = jax.ShapeDtypeStruct((half, width), jnp.float32)
    slot = [jax.ShapeDtypeStruct((n, lanes), jnp.float32) for n in (groups, lanes, groups)]
    place = (row_start.reshape(1), core.reshape(1))

    sent, high, low, factor, most, repeated, rank, code = pl.pallas_call(
        send_kernel,
        out_shape=(
            pools,
            *slot,
            jax.ShapeDtypeStruct((8, lanes), jnp.float32),
            jax.ShapeDtypeStruct((tiles // 2, lanes), jnp.float32),
            by_position,
            by_position,
        ),
        in_specs=[smem, smem, far, far, far, far],
        out_specs=(vmem,) * 8,
        scratch_shapes=scratch,
        compiler_params=limit,
    )(*place, index_rows, weight, length, table_rows)

    def keep():
        return pl.pallas_call(
            keep_kernel,
            out_shape=pools,
            in_specs=[smem, smem, vmem, vmem, vmem, vmem, vmem, vmem, vmem, far],
            out_specs=vmem,
            scratch_shapes=[table_scratch, *by_group, spread, dma],
            compiler_params=limit,
            cost_estimate=pl.CostEstimate(
                flops=8 * half * rows * width, bytes_accessed=rows * width * 2, transcendentals=0
            ),
        )(*place, most, repeated, rank, code, high, low, factor, table_rows)

    return sent, keep


def on_device(tables, indices, weights, lengths):
    _, row_dev, feature_width = tables.shape
    batch_size = indices.shape[2]
    table_count = lax.axis_size("table")
    pair_count = lax.axis_size("pair")
    core = lax.axis_index("core").astype(jnp.int32)
    row = lax.axis_index("pair").astype(jnp.int32) * 2 + core
    index_rows = indices.transpose(1, 0, 2)
    sent, keep = kernels(tables[0], index_rows, weights[0], lengths, row * row_dev, core)
    received = lax.ppermute(sent, "core", [(0, 1), (1, 0)])
    partial = keep() + received
    share = batch_size // (table_count * pair_count * 2)
    tiles = partial.reshape(table_count * pair_count, share, feature_width)
    groups = [
        [(t * pair_count + (p ^ far_pair)) * 2 + c for t in range(table_count) for p in range(pair_count)]
        for c in range(2)
    ]
    arrived = lax.all_to_all(
        tiles,
        ("table", "pair", "core"),
        split_axis=0,
        concat_axis=0,
        axis_index_groups=groups,
        tiled=True,
    )
    shares = arrived.reshape(table_count, pair_count, share, feature_width)
    return shares.sum(axis=1).astype(jnp.bfloat16)


def solution(mesh):
    tables, rows = mesh.devices.shape
    by_core = Mesh(mesh.devices.reshape(tables, rows // 2, 2), ("table", "pair", "core"))
    row = ("pair", "core")
    placed = (
        P("table", row, None),
        P("table", None, None),
        P("table", None, None),
        P("table", None),
    )
    return jax.shard_map(
        on_device,
        mesh=by_core,
        in_specs=placed,
        out_specs=P(None, ("table", *row), None),
        check_vma=False,
    )
```

```python
import functools

import jax
import jax.numpy as jnp
from jax import lax
from jax.experimental import pallas as pl
from jax.experimental.pallas import tpu as pltpu
from jax.sharding import Mesh
from jax.sharding import PartitionSpec as P

lanes = 128
packed_rows = 16
slots = 16
weight_unit = 1024
far_pair = 26
vmem_bytes = 20 * 2**20


def read_positions(start_ref, index_ref, weight_ref, length_ref, rank_ref, code_ref, rows):
    bag, _, batch = index_ref.shape
    padded = rank_ref.shape[0]
    local = index_ref[:, 0, :] - start_ref[0]
    position = lax.broadcasted_iota(jnp.int32, (bag, batch), 0)
    inside = (local >= 0) & (local < rows) & (position < length_ref[...])
    code = local.astype(jnp.float32) * (2.0 * weight_unit)
    code = code + weight_ref[...].astype(jnp.float32) * weight_unit
    code_ref[:bag, :] = jnp.where(inside, code, 0.0)
    code_ref[bag:, :] = jnp.zeros((padded - bag, batch), jnp.float32)

    used = jnp.where(inside, 1.0, 0.0)
    used = jnp.concatenate([used, jnp.zeros((lanes - bag, batch), jnp.float32)], 0)
    before = lax.broadcasted_iota(jnp.int32, (padded, lanes), 0) > lax.broadcasted_iota(
        jnp.int32, (padded, lanes), 1
    )
    rank = jnp.dot(
        jnp.where(before, 1.0, 0.0).astype(jnp.bfloat16),
        used.astype(jnp.bfloat16),
        preferred_element_type=jnp.float32,
    )
    rank_ref[...] = rank
    return jnp.max(rank[padded - 1 :, :], keepdims=True)


def rounds_for(most):
    return (jnp.max(most).astype(jnp.int32) + (slots - 1)) // slots


def note_repeats(plane, repeated_ref):
    row = (plane.astype(jnp.int32) // (2 * weight_unit)).astype(jnp.float32)
    slot = lax.broadcasted_iota(jnp.int32, plane.shape, 0).astype(jnp.float32)
    row = jnp.where(plane > 0, row, -1.0 - slot)
    noted = []
    for first in range(0, plane.shape[0], slots):
        rows = row[first : first + slots]
        again = jnp.full(rows.shape, -1.0, jnp.float32)
        for shift in range(1, slots // 2 + 1):
            again = jnp.where(rows == pltpu.roll(rows, shift, 0), rows, again)
        noted.append((again.astype(jnp.int32) >> 8).astype(jnp.float32))
    for pair in range(repeated_ref.shape[0]):
        repeated_ref[pair : pair + 1, :] = any_in_pair(noted, pair)


def any_in_pair(noted, pair):
    hits = [jnp.where(pairs == float(pair), 1.0, 0.0) for pairs in noted]
    return jnp.max(functools.reduce(jnp.maximum, hits), axis=0, keepdims=True)


def note_later(plane, repeated_ref):
    pairs = (plane.astype(jnp.int32) // (2 * weight_unit)) >> 8
    noted = [jnp.where(plane > 0, pairs.astype(jnp.float32), -1.0)]
    for pair in range(repeated_ref.shape[0]):
        where = slice(pair, pair + 1)
        repeated_ref[where, :] = jnp.maximum(repeated_ref[where, :], any_in_pair(noted, pair))


def fill_slots(rank_ref, code_ref, slot_refs, first):
    high_ref, low_ref, factor_ref = slot_refs
    groups = high_ref.shape[0]
    planes = []
    for block in range(rank_ref.shape[1] // lanes):
        where = pl.ds(block * lanes, lanes)
        rank = rank_ref[:, where]
        code = code_ref[:, where]
        for s in range(slots):
            at = rank == (first + s).astype(jnp.float32)
            planes.append(jnp.sum(jnp.where(at, code, 0.0), axis=0, keepdims=True))
    slot_codes = jnp.concatenate(planes, 0)
    plane = jnp.concatenate([slot_codes, pltpu.roll(slot_codes, lanes - groups, 1)], 0)
    low_ref[...] = (plane.astype(jnp.int32) // (2 * weight_unit) % lanes).astype(jnp.float32)
    code = plane.T[:groups].astype(jnp.int32)
    row = code // (2 * weight_unit)
    high_ref[...] = (row // lanes).astype(jnp.float32)
    factor = (code % (2 * weight_unit)).astype(jnp.float32)
    factor_ref[...] = factor * (1.0 / weight_unit)
    return slot_codes


def spread_half(slot_refs, spread_ref, core, tiles, add):
    high_ref, low_ref, factor_ref = slot_refs
    group_bags = lanes // slots
    half_groups = high_ref.shape[0] // 2
    stride = spread_ref.shape[0] // tiles
    row_id = lax.broadcasted_iota(jnp.int32, (packed_rows, lanes), 0)
    row_ids = [
        (row_id + packed_rows * i).astype(jnp.float32).astype(jnp.bfloat16)
        for i in range(tiles // packed_rows)
    ]
    zero = jnp.zeros((packed_rows, lanes), jnp.bfloat16)
    lane = lax.broadcasted_iota(jnp.int32, (lanes, lanes), 1).astype(jnp.float32)
    lows = pltpu.roll(low_ref[...], (lanes - 2 * core) % lanes, 1)
    owner = lax.broadcasted_iota(jnp.int32, (packed_rows, lanes), 1) // slots
    owner = owner.astype(jnp.float32).astype(jnp.bfloat16)
    owned = [owner == jnp.full_like(owner, g) for g in range(group_bags)]

    def row_of(ref, j):
        row = ref[pl.ds(j, 1), :]
        return jnp.broadcast_to(row, (packed_rows, lanes)).astype(jnp.bfloat16)

    def spread_group(t):
        j = t // 2 * 4 + t % 2 + 2 * core
        high = row_of(high_ref, j)
        factor = row_of(factor_ref, j)
        at = [high == ids for ids in row_ids]
        by_high = []
        for g in range(group_bags):
            mine = jnp.where(owned[g], factor, zero)
            by_high += [jnp.where(hit, mine, zero) for hit in at]
        at_lane = t // 2 * 4 + t % 2
        low = jnp.broadcast_to(lows[:, at_lane : at_lane + 1], (lanes, lanes))
        by_low = jnp.where(low == lane, 1.0, 0.0).astype(jnp.bfloat16)
        total = lax.dot_general(
            jnp.concatenate(by_high, 0),
            by_low,
            (((1,), (0,)), ((), ())),
            preferred_element_type=jnp.float32,
        )
        blocks = group_bags // 2
        for g in range(group_bags):
            pair = (g // blocks * half_groups + t) // 2 ^ far_pair
            bag = g % blocks * 2 * half_groups + pair * 2 + t % 2
            where = pl.ds(bag, tiles, stride=stride)
            part = total[g * tiles : (g + 1) * tiles]
            if add:
                part = part + spread_ref[where, :]
            spread_ref[where, :] = part

    numbers = range(half_groups)
    if add:
        found = [jnp.max(factor_ref[pl.ds(t // 2 * 4 + t % 2 + 2 * core, 1), :]) for t in numbers]
        for t in numbers:
            pl.when(found[t] > 0)(functools.partial(spread_group, t))
    else:
        for t in numbers:
            spread_group(t)


def multiply(spread_ref, table_ref, repeated_ref, core, out_ref):
    tiles = table_ref.shape[0] // lanes
    stride = spread_ref.shape[0] // tiles
    bags = out_ref.shape[0]
    lane = lax.broadcasted_iota(jnp.int32, (1, lanes), 1)
    ours = (lane // 2) % 2 == core
    left = [
        jnp.where(ours, repeated_ref[pair : pair + 1, :], 0.0) for pair in range(tiles // 2)
    ]
    left_in_four = [
        jnp.max(functools.reduce(jnp.maximum, left[i : i + 4])) > 0 for i in range(0, len(left), 4)
    ]
    left = [jnp.max(some) > 0 for some in left]
    factors = [
        spread_ref[pl.ds(i * stride, bags), :].astype(jnp.bfloat16) for i in range(tiles)
    ]
    out_ref[...] = jnp.dot(
        jnp.concatenate(factors, 1), table_ref[...], preferred_element_type=jnp.float32
    )

    def add_rest(pair):
        factors = [spread_ref[pl.ds((2 * pair + i) * stride, bags), :] for i in range(2)]
        factors = jnp.concatenate(factors, 1)
        rest = factors - factors.astype(jnp.bfloat16).astype(jnp.float32)
        out_ref[...] += jnp.dot(
            rest.astype(jnp.bfloat16),
            table_ref[pl.ds(2 * pair * lanes, 2 * lanes), :],
            preferred_element_type=jnp.float32,
        )

    for four in range(tiles // 8):

        @pl.when(left_in_four[four])
        def _(four=four):
            for pair in range(4 * four, 4 * four + 4):
                pl.when(left[pair])(functools.partial(add_rest, pair))


def send_kernel(
    start_ref,
    core_ref,
    index_hbm,
    weight_hbm,
    length_hbm,
    table_hbm,
    out_ref,
    high_ref,
    low_ref,
    factor_ref,
    most_ref,
    repeated_ref,
    rank_ref,
    code_ref,
    table_ref,
    index_ref,
    weight_ref,
    length_ref,
    high_later,
    low_later,
    factor_later,
    spread_ref,
    table_sem,
    index_sem,
    weight_sem,
    length_sem,
):
    half_bag = index_ref.shape[0] // 2
    copies = [
        *[
            pltpu.make_async_copy(
                index_hbm.at[pl.ds(part * half_bag, half_bag)],
                index_ref.at[pl.ds(part * half_bag, half_bag)],
                index_sem.at[part],
            )
            for part in range(2)
        ],
        pltpu.make_async_copy(weight_hbm, weight_ref, weight_sem),
        pltpu.make_async_copy(length_hbm, length_ref, length_sem),
    ]
    for copy in copies:
        copy.start()
    for copy in copies:
        copy.wait()
    table_copy = pltpu.make_async_copy(table_hbm, table_ref, table_sem)
    table_copy.start()
    rows = table_ref.shape[0]
    tiles = rows // lanes
    core = 1 - core_ref[0]
    most = read_positions(
        start_ref, index_ref, weight_ref, length_ref, rank_ref, code_ref, rows
    )
    most_ref[...] = jnp.broadcast_to(most, most_ref.shape)
    rounds = rounds_for(most)
    slot_refs = (high_ref, low_ref, factor_ref)
    later_refs = (high_later, low_later, factor_later)
    plane = fill_slots(rank_ref, code_ref, slot_refs, jnp.int32(0))
    spread_half(slot_refs, spread_ref, core, tiles, False)
    note_repeats(plane, repeated_ref)

    def later_round(number, carry):
        note_later(fill_slots(rank_ref, code_ref, later_refs, number * slots), repeated_ref)
        spread_half(later_refs, spread_ref, core, tiles, True)
        return carry

    lax.fori_loop(1, rounds, later_round, 0)
    table_copy.wait()
    multiply(spread_ref, table_ref, repeated_ref, core, out_ref)


def keep_kernel(
    start_ref,
    core_ref,
    most_ref,
    repeated_ref,
    rank_ref,
    code_ref,
    high_ref,
    low_ref,
    factor_ref,
    table_hbm,
    out_ref,
    table_ref,
    high_later,
    low_later,
    factor_later,
    spread_ref,
    table_sem,
):
    table_copy = pltpu.make_async_copy(table_hbm, table_ref, table_sem)
    table_copy.start()
    rows = table_ref.shape[0]
    tiles = rows // lanes
    core = core_ref[0]
    slot_refs = (high_ref, low_ref, factor_ref)
    later_refs = (high_later, low_later, factor_later)
    spread_half(slot_refs, spread_ref, core, tiles, False)
    rounds = rounds_for(most_ref[...])

    def later_round(number, carry):
        fill_slots(rank_ref, code_ref, later_refs, number * slots)
        spread_half(later_refs, spread_ref, core, tiles, True)
        return carry

    lax.fori_loop(1, rounds, later_round, 0)
    table_copy.wait()
    multiply(spread_ref, table_ref, repeated_ref, core, out_ref)


def kernels(table_rows, index_rows, weight, length, row_start, core):
    rows, width = table_rows.shape
    bag, batch = weight.shape
    padded = bag + 8 - bag % 8
    groups = batch * slots // lanes
    half = batch // 2
    tiles = rows // lanes
    smem = pl.BlockSpec(memory_space=pltpu.SMEM)
    vmem = pl.BlockSpec(memory_space=pltpu.VMEM)
    far = pl.BlockSpec(memory_space=pl.ANY)
    table_scratch = pltpu.VMEM((rows, width), table_rows.dtype)
    by_position = jax.ShapeDtypeStruct((padded, batch), jnp.float32)
    by_group = [pltpu.VMEM((n, lanes), jnp.float32) for n in (groups, lanes, groups)]
    spread = pltpu.VMEM(((half + 1) * tiles, lanes), jnp.float32)
    dma = pltpu.SemaphoreType.DMA
    scratch = [
        table_scratch,
        pltpu.VMEM(index_rows.shape, index_rows.dtype),
        pltpu.VMEM(weight.shape, weight.dtype),
        pltpu.VMEM(length.shape, length.dtype),
        *by_group,
        spread,
        dma,
        dma((2,)),
        dma,
        dma,
    ]
    limit = pltpu.CompilerParams(vmem_limit_bytes=vmem_bytes)
    index_rows, weight, length, table_rows = [
        pltpu.with_memory_space_constraint(value, pltpu.HBM)
        for value in (index_rows, weight, length, table_rows)
    ]
    pools = jax.ShapeDtypeStruct((half, width), jnp.float32)
    slot = [jax.ShapeDtypeStruct((n, lanes), jnp.float32) for n in (groups, lanes, groups)]
    place = (row_start.reshape(1), core.reshape(1))

    sent, high, low, factor, most, repeated, rank, code = pl.pallas_call(
        send_kernel,
        out_shape=(
            pools,
            *slot,
            jax.ShapeDtypeStruct((8, lanes), jnp.float32),
            jax.ShapeDtypeStruct((tiles // 2, lanes), jnp.float32),
            by_position,
            by_position,
        ),
        in_specs=[smem, smem, far, far, far, far],
        out_specs=(vmem,) * 8,
        scratch_shapes=scratch,
        compiler_params=limit,
    )(*place, index_rows, weight, length, table_rows)

    def keep():
        return pl.pallas_call(
            keep_kernel,
            out_shape=pools,
            in_specs=[smem, smem, vmem, vmem, vmem, vmem, vmem, vmem, vmem, far],
            out_specs=vmem,
            scratch_shapes=[table_scratch, *by_group, spread, dma],
            compiler_params=limit,
            cost_estimate=pl.CostEstimate(
                flops=8 * half * rows * width, bytes_accessed=rows * width * 2, transcendentals=0
            ),
        )(*place, most, repeated, rank, code, high, low, factor, table_rows)

    return sent, keep


def on_device(tables, indices, weights, lengths):
    _, row_dev, feature_width = tables.shape
    batch_size = indices.shape[2]
    table_count = lax.axis_size("table")
    pair_count = lax.axis_size("pair")
    core = lax.axis_index("core").astype(jnp.int32)
    row = lax.axis_index("pair").astype(jnp.int32) * 2 + core
    index_rows = indices.transpose(1, 0, 2)
    sent, keep = kernels(tables[0], index_rows, weights[0], lengths, row * row_dev, core)
    received = lax.ppermute(sent, "core", [(0, 1), (1, 0)])
    partial = keep() + received
    share = batch_size // (table_count * pair_count * 2)
    tiles = partial.reshape(table_count * pair_count, share, feature_width)
    groups = [
        [(t * pair_count + (p ^ far_pair)) * 2 + c for t in range(table_count) for p in range(pair_count)]
        for c in range(2)
    ]
    arrived = lax.all_to_all(
        tiles,
        ("table", "pair", "core"),
        split_axis=0,
        concat_axis=0,
        axis_index_groups=groups,
        tiled=True,
    )
    shares = arrived.reshape(table_count, pair_count, share, feature_width)
    return shares.sum(axis=1).astype(jnp.bfloat16)


def solution(mesh):
    tables, rows = mesh.devices.shape
    by_core = Mesh(mesh.devices.reshape(tables, rows // 2, 2), ("table", "pair", "core"))
    row = ("pair", "core")
    placed = (
        P("table", row, None),
        P("table", None, None),
        P("table", None, None),
        P("table", None),
    )
    return jax.shard_map(
        on_device,
        mesh=by_core,
        in_specs=placed,
        out_specs=P(None, ("table", *row), None),
        check_vma=False,
    )
```
